32 devices in a mesh: members: 2 (over y), band: 4 (over z), head: 4 (over x, core).
Axes of the slice: x: 2, y: 2, z: 4, core: 2. Of those that a mesh axis runs over, the one named last changes fastest.
Arguments:
- grid_feats: bfloat16 [4096, 1024], P(('members', 'band')), parts along dimension 0, may hold values from -6 to 6
- mesh_feats: bfloat16 [4096, 1024], P(('members', 'band')), parts along dimension 0, may hold values from -6 to 6
- enc_in: bfloat16 [3, 1024, 1024], P(None, 'band', 'head'), may hold values from -0.19921875 to 0.19921875
- enc_out: bfloat16 [1024, 1024], P('head', 'band'), may hold values from -0.1875 to 0.1875
- proc_in: bfloat16 [3, 1024, 1024], P(None, 'band', 'head'), may hold values from -0.19921875 to 0.19921875
- proc_out: bfloat16 [1024, 1024], P('head', 'band'), may hold values from -0.1875 to 0.1875
- ff_up: bfloat16 [1024, 4096], P('band', 'head'), may hold values from -0.1875 to 0.1875
- ff_down: bfloat16 [4096, 1024], P('head', 'band'), may hold values from -0.09375 to 0.09375
- dec_in: bfloat16 [3, 1024, 1024], P(None, 'band', 'head'), may hold values from -0.19921875 to 0.19921875
- dec_out: bfloat16 [1024, 1024], P('head', 'band'), may hold values from -0.1875 to 0.1875
- enc_list: int32 [16, 8], replicated, may hold values from 0 to 15, as said below
- enc_count: int32 [16], replicated, may hold values from 1 to 8
- dec_list: int32 [16, 8], replicated, may hold values from 0 to 15, as said below
- dec_count: int32 [16], replicated, may hold values from 1 to 8
- window_ids: int32 [2048], replicated, may hold values from 0 to 1, never falling along the last dimension, each value on 1 to 1536 neighbouring positions
Outputs:
- grid_out: bfloat16 [4096, 1024], P(('members', 'band', 'head')), parts along dimension 0
The draws below stay inside these ranges and needn't reach their ends.
There are 2 independent parts, one for each index of `members`. The reference program is written for one: setup_inputs(seed, part) draws one part's arguments, and reference() takes and returns one part's arrays. A program takes and returns all parts, laid end to end along the dimension named above; an argument that names none is the same for every part. Nothing has to cross between parts.
Inputs may be any that keep to these rules, and one draw needn't show every extreme that they name: `enc_list`: each row holds distinct block numbers. Every block listed for mesh block m lies in the band of 512 grid points with the same band number as m's band of 512 nodes, or in the band just before or just after it. Only the first enc_count[m] slots of row m of enc_list are used. `dec_list`: each row holds distinct block numbers. Every block listed for grid block g lies in the band of 512 mesh nodes with the same band number as g's band of 512 grid points, or in the band just before or just after it. Only the first dec_count[g] slots of row g of dec_list are used. `window_ids`: never falls along the nodes; each window holds at most 1536 consecutive nodes.
All inputs are finite; a program needn't handle non-finite values.
Results may differ from the reference program's by a relative error of at most 0.02.
Values may be sent and summed in bfloat16 or wider, within the bound.
No kernel may reach another device: no remote copies, remote signals or barrier semaphores. Data moves between devices by JAX's collectives and lax.ppermute only.
A program may use at most 64 MiB of HBM per device.

```python
import math
import jax
import jax.numpy as jnp
import numpy as np
from jax import lax

D = 1024
HEADS = 16
FF = 4096
HD = 64
BLOCK = 128
LIST = 8
WINDOW = 1536
GRID_DEV = 512
MESH_DEV = 512
GRID = 2048
MESH = 2048
WINDOWS = 2
N_HEAD = 4


def block_choice(key, query_blocks, query_per_band, cand_per_band, cand_total):
    band_of = jnp.arange(query_blocks, dtype=jnp.int32) // query_per_band
    offsets = jnp.arange(3 * cand_per_band, dtype=jnp.int32)
    candidates = (band_of[:, None] - 1) * cand_per_band + offsets[None, :]
    usable = (candidates >= 0) & (candidates < cand_total)
    scores = jax.random.randint(key, (query_blocks, 3 * cand_per_band), 0, 1 << 20, dtype=jnp.int32)
    scores = scores * (3 * cand_per_band) + offsets[None, :]
    scores = jnp.where(usable, scores, (1 << 30) + offsets[None, :])
    order = jnp.argsort(scores, axis=1, stable=True)
    picked = jnp.take_along_axis(candidates, order[:, :LIST], axis=1)
    return picked.astype(jnp.int32)


def draw_enc_list(key, part):
    return block_choice(jax.random.fold_in(key, 11), MESH // BLOCK, MESH_DEV // BLOCK, GRID_DEV // BLOCK, GRID // BLOCK)


def draw_dec_list(key, part):
    return block_choice(jax.random.fold_in(key, 23), GRID // BLOCK, GRID_DEV // BLOCK, MESH_DEV // BLOCK, MESH // BLOCK)


def projection_base(key):
    return jax.random.truncated_normal(key, -6.0, 6.0, (3, D, D), jnp.float32) * D ** (-0.5)


def state_base(key, count):
    return jax.random.truncated_normal(key, -6.0, 6.0, (count, D), jnp.float32)


def draw_enc_in(key, part):
    base = projection_base(jax.random.fold_in(key, 31))
    return base.astype(jnp.bfloat16)


def draw_proc_in(key, part):
    base = projection_base(jax.random.fold_in(key, 37))
    return base.astype(jnp.bfloat16)


def draw_dec_in(key, part):
    base = projection_base(jax.random.fold_in(key, 41))
    return base.astype(jnp.bfloat16)


def draw_grid_feats(key, part):
    base = state_base(jax.random.fold_in(key, 43), GRID)
    return base.astype(jnp.bfloat16)


def draw_mesh_feats(key, part):
    base = state_base(jax.random.fold_in(key, 53), MESH)
    return base.astype(jnp.bfloat16)


def plant(array, stream_key, low, largest):
    extent = array.shape
    place = [jax.random.randint(jax.random.fold_in(stream_key, axis), (), 0, extent[axis]) for axis in range(len(extent))]
    array = array.at[tuple(place)].set(low)
    longest = extent.index(max(extent))
    place[longest] = (place[longest] + 1) % extent[longest]
    return array.at[tuple(place)].set(largest)


def levels(rng, dims, pieces, smallest, high):
    gain = 1.0
    for position, shards_of in pieces:
        steps = jax.random.uniform(jax.random.fold_in(jax.random.fold_in(rng, 6), position), (shards_of,), jnp.float32, smallest / len(pieces), high / len(pieces))
        gain = gain * jnp.repeat(jnp.exp(steps), dims[position] // shards_of).reshape((-1,) + (1,) * (len(dims) - 1 - position))
    return gain


def profile(number_of, total, limit, slope):
    portions = [(1 << 20) // math.isqrt(rank ** slope) + 1 for rank in range(2, number_of + 1)]
    surplus, given = total - limit - (number_of - 1), [1] * (number_of - 1)
    while surplus > 0:
        free = [i for i in range(number_of - 1) if given[i] < limit]
        whole, budget = sum([portions[i] for i in free]), surplus
        for i in free:
            more = min(limit - given[i], max(1, budget * portions[i] // whole), surplus)
            given[i] = given[i] + more
            surplus = surplus - more
    return np.array([limit] + given)


def uneven_parts(stream_key, amount, total, reach, lean):
    if amount == 2:
        one = jax.random.randint(stream_key, (), max(1, total - reach), min(reach, total - 1) + 1)
        return jnp.stack([one, total - one])
    tallies = jnp.asarray(profile(amount, total, reach, lean), jnp.int32)
    couples = (amount - 1) // 2
    giver, taker = tallies[1:1 + 2 * couples:2], tallies[2:2 + 2 * couples:2]
    room = jnp.minimum(giver - 1, reach - taker)
    passed = jax.random.randint(jax.random.fold_in(stream_key, 1), (couples,), 0, 1 << 20) % (room + 1)
    tallies = tallies.at[1:1 + 2 * couples:2].set(giver - passed).at[2:2 + 2 * couples:2].set(taker + passed)
    return tallies[jax.random.permutation(jax.random.fold_in(stream_key, 2), amount)]


def normal_values(key, dims, width, limit, split=(), kind=jnp.bfloat16):
    values = jax.random.normal(key, dims, jnp.float32) * width
    if len(split) > 0:
        values = levels(key, dims, split, -0.22, 0.18) * values
    return jnp.clip(values, min=-limit, max=limit).astype(kind)


def setup_inputs(seed: int = 0, part: int = 0) -> dict:
    key_of = jax.random.split(jax.random.key(seed), 16)
    part_keys = jax.random.split(jax.random.fold_in(key_of[15], part), 16)
    grid_feats = draw_grid_feats(jax.random.fold_in(jax.random.fold_in(key_of[15], part), 71), part)
    mesh_feats = draw_mesh_feats(jax.random.fold_in(jax.random.fold_in(key_of[15], part), 71), part)
    enc_in = draw_enc_in(jax.random.fold_in(key_of[15], 71), part)
    enc_out = normal_values(key_of[3], (D, D), D ** -0.5, 0.1875, ((0, 4), (1, 4)))
    proc_in = draw_proc_in(jax.random.fold_in(key_of[15], 71), part)
    proc_out = normal_values(key_of[5], (D, D), D ** -0.5, 0.1875, ((0, 4), (1, 4)))
    ff_up = normal_values(key_of[6], (D, FF), D ** -0.5, 0.1875, ((0, 4), (1, 4)))
    ff_down = normal_values(key_of[7], (FF, D), FF ** -0.5, 0.09375, ((0, 4), (1, 4)))
    dec_in = draw_dec_in(jax.random.fold_in(key_of[15], 71), part)
    dec_out = normal_values(key_of[9], (D, D), D ** -0.5, 0.1875, ((0, 4), (1, 4)))
    enc_list = draw_enc_list(jax.random.fold_in(key_of[15], 71), part)
    enc_count = plant(jax.random.randint(key_of[11], (MESH // BLOCK,), 1, LIST + 1), jax.random.fold_in(key_of[11], 1), 1, LIST).astype(jnp.int32)
    dec_list = draw_dec_list(jax.random.fold_in(key_of[15], 71), part)
    dec_count = plant(jax.random.randint(key_of[13], (GRID // BLOCK,), 1, LIST + 1), jax.random.fold_in(key_of[13], 1), 1, LIST).astype(jnp.int32)
    window_ids = jnp.searchsorted(jnp.cumsum(uneven_parts(key_of[14], WINDOWS, MESH, WINDOW, 0)), jnp.arange(MESH), side="right").astype(jnp.int32)
    return {"grid_feats": grid_feats, "mesh_feats": mesh_feats, "enc_in": enc_in, "enc_out": enc_out, "proc_in": proc_in, "proc_out": proc_out, "ff_up": ff_up, "ff_down": ff_down, "dec_in": dec_in, "dec_out": dec_out, "enc_list": enc_list, "enc_count": enc_count, "dec_list": dec_list, "dec_count": dec_count, "window_ids": window_ids}


EPSILON = 1e-05
NEGATIVE = -1e+30
HIGHEST = lax.Precision.HIGHEST

def normed(source):
    values_f = source.astype(jnp.float32)
    centred = values_f - lax.optimization_barrier(jnp.mean(values_f, axis=-1, keepdims=True))
    variance = lax.optimization_barrier(jnp.mean(centred * centred, axis=-1, keepdims=True))
    return (centred * lax.rsqrt(variance + EPSILON)).astype(jnp.bfloat16)

def project(source, weight):
    return jnp.dot(source, weight, preferred_element_type=jnp.float32).astype(jnp.bfloat16)

def group_sum(source, weight):
    inner = source.shape[1] // N_HEAD
    total = jnp.zeros((source.shape[0], weight.shape[1]), jnp.float32)
    for group in range(N_HEAD):
        part_sum = jnp.dot(source[:, group * inner:(group + 1) * inner], weight[group * inner:(group + 1) * inner], preferred_element_type=jnp.float32)
        rounded = lax.optimization_barrier(part_sum.astype(jnp.bfloat16))
        total = total + rounded.astype(jnp.float32)
    return total

def split_heads(rows):
    return rows.astype(jnp.float32).reshape(rows.shape[0], HEADS, HD)

def softmax_parts(queries, key_rows, allowed):
    scores = jnp.einsum('qhd,khd->hqk', split_heads(queries), split_heads(key_rows), precision=HIGHEST) * HD ** (-0.5)
    scores = jnp.where(allowed[None], scores, NEGATIVE)
    maxima = lax.optimization_barrier(jnp.max(scores, axis=-1, keepdims=True))
    expo = jnp.exp(scores - maxima) * allowed[None].astype(jnp.float32)
    return (expo, lax.optimization_barrier(jnp.sum(expo, axis=-1, keepdims=True)))

def listed_attention(queries, key_rows, value_rows, lists, counts, rounded_weights):
    key_blocks = key_rows.reshape(key_rows.shape[0] // BLOCK, BLOCK, D)
    value_blocks = value_rows.reshape(value_rows.shape[0] // BLOCK, BLOCK, D)

    def one_block(index):
        listed = lists[index]
        live = jnp.arange(LIST, dtype=jnp.int32) < counts[index]
        block_keys = key_blocks[listed].reshape(LIST * BLOCK, D)
        block_values = value_blocks[listed].reshape(LIST * BLOCK, D)
        allowed = jnp.repeat(live, BLOCK)[None, :]
        block_queries = lax.dynamic_slice_in_dim(queries, index * BLOCK, BLOCK, 0)
        expo, totals = softmax_parts(block_queries, block_keys, allowed)
        if rounded_weights:
            weights = (expo / totals).astype(jnp.bfloat16).astype(jnp.float32)
            mixed = jnp.einsum('hqk,khd->qhd', weights, split_heads(block_values), precision=HIGHEST)
        else:
            mixed = jnp.einsum('hqk,khd->qhd', expo, split_heads(block_values), precision=HIGHEST)
            mixed = mixed / jnp.transpose(totals, (1, 0, 2))
        return mixed.reshape(BLOCK, D).astype(jnp.bfloat16)
    blocks = lax.map(one_block, jnp.arange(queries.shape[0] // BLOCK, dtype=jnp.int32))
    return blocks.reshape(queries.shape[0], D)

def window_attention(queries, key_rows, value_rows, window_ids):
    padded_keys = jnp.pad(key_rows, ((WINDOW, WINDOW), (0, 0)))
    padded_values = jnp.pad(value_rows, ((WINDOW, WINDOW), (0, 0)))
    padded_ids = jnp.pad(window_ids, (WINDOW, WINDOW), constant_values=-1)

    def one_block(index):
        start = index * BLOCK
        block_queries = lax.dynamic_slice_in_dim(queries, start, BLOCK, 0)
        block_keys = lax.dynamic_slice_in_dim(padded_keys, start, BLOCK + 2 * WINDOW, 0)
        block_values = lax.dynamic_slice_in_dim(padded_values, start, BLOCK + 2 * WINDOW, 0)
        key_ids = lax.dynamic_slice_in_dim(padded_ids, start, BLOCK + 2 * WINDOW, 0)
        query_ids = lax.dynamic_slice_in_dim(window_ids, start, BLOCK, 0)
        allowed = query_ids[:, None] == key_ids[None, :]
        expo, totals = softmax_parts(block_queries, block_keys, allowed)
        weights = (expo / totals).astype(jnp.bfloat16).astype(jnp.float32)
        mixed = jnp.einsum('hqk,khd->qhd', weights, split_heads(block_values), precision=HIGHEST)
        return mixed.reshape(BLOCK, D).astype(jnp.bfloat16)
    blocks = lax.map(one_block, jnp.arange(queries.shape[0] // BLOCK, dtype=jnp.int32))
    return blocks.reshape(queries.shape[0], D)

def reference(grid_feats, mesh_feats, enc_in, enc_out, proc_in, proc_out, ff_up, ff_down, dec_in, dec_out, enc_list, enc_count, dec_list, dec_count, window_ids):
    grid_norm = normed(grid_feats)
    mesh_norm = normed(mesh_feats)
    enc_q = project(mesh_norm, enc_in[0])
    enc_k = project(grid_norm, enc_in[1])
    enc_v = project(grid_norm, enc_in[2])
    enc_attn = listed_attention(enc_q, enc_k, enc_v, enc_list, enc_count, False)
    mesh_state = mesh_feats.astype(jnp.float32) + group_sum(enc_attn, enc_out)
    proc_norm = normed(mesh_state)
    proc_q = project(proc_norm, proc_in[0])
    proc_k = project(proc_norm, proc_in[1])
    proc_v = project(proc_norm, proc_in[2])
    proc_attn = window_attention(proc_q, proc_k, proc_v, window_ids)
    mesh_mid = mesh_state + group_sum(proc_attn, proc_out)
    hidden = jax.nn.gelu(jnp.dot(normed(mesh_mid), ff_up, preferred_element_type=jnp.float32), approximate=False).astype(jnp.bfloat16)
    mesh_final = mesh_mid + group_sum(hidden, ff_down)
    final_norm = normed(mesh_final)
    dec_q = project(grid_norm, dec_in[0])
    dec_k = project(final_norm, dec_in[1])
    dec_v = project(final_norm, dec_in[2])
    dec_attn = listed_attention(dec_q, dec_k, dec_v, dec_list, dec_count, True)
    return (grid_feats.astype(jnp.float32) + group_sum(dec_attn, dec_out)).astype(jnp.bfloat16)
```

```python
import functools

import jax
import jax.numpy as jnp
from jax import lax
from jax.experimental import pallas as pl
from jax.experimental.pallas import tpu as pltpu
from jax.sharding import PartitionSpec as P

HD = 64
BLOCK = 128
WINDOW = 1536
LANES = 128

EPSILON = 1e-05
NEGATIVE = -1e30


def dot(a, b):
    return jnp.dot(a, b, preferred_element_type=jnp.float32)


def normed(values):
    values = values.astype(jnp.float32)
    centred = values - jnp.mean(values, axis=-1, keepdims=True)
    variance = jnp.mean(centred * centred, axis=-1, keepdims=True)
    return (centred * lax.rsqrt(variance + EPSILON)).astype(jnp.bfloat16)


def exchange(value, axis, bit):
    count = lax.axis_size(axis)
    return lax.ppermute(value, axis, [(i, i ^ bit) for i in range(count)])


def half_shard(weight, members):
    rows = weight.shape[0] // members
    return lax.dynamic_slice_in_dim(weight, lax.axis_index("members") * rows, rows, 0)


def gather(value):
    members, bands = lax.axis_size("members"), lax.axis_size("band")
    whole = lax.all_gather(value, ("members", "band"), axis=0, tiled=False)
    return whole.reshape((members, bands) + value.shape)


def by_rows(pieces):
    members, bands, rows, columns = pieces.shape
    return pieces.transpose(1, 0, 2, 3).reshape(bands * members * rows, columns)


def by_columns(pieces):
    members, bands, rows, columns = pieces.shape
    return pieces.transpose(0, 2, 1, 3).reshape(members * rows, bands * columns)


def gather_projections(w_in, w_out):
    members = lax.axis_size("members")
    k_rows = w_in.shape[1] // members
    o_rows = w_out.shape[0] // members
    member = lax.axis_index("members")
    part_in = lax.dynamic_slice_in_dim(w_in, member * k_rows, k_rows, 1)
    part_out = half_shard(w_out, members)
    width = w_in.shape[2]
    flat_in = part_in.reshape(3 * k_rows, width)
    flat_out = part_out.reshape(-1, width)
    pieces = gather(jnp.concatenate([flat_in, flat_out], axis=0))
    bands = pieces.shape[1]
    mats = [by_rows(pieces[:, :, i * k_rows : (i + 1) * k_rows]) for i in range(3)]
    outs = pieces[:, :, 3 * k_rows :].reshape(members, bands, o_rows, w_out.shape[1])
    return mats, by_columns(outs)


def attention_kernel(pieces, keyed, *refs):
    q_ref = refs[0]
    kv_refs = refs[1 : 1 + pieces]
    mask_refs = refs[1 + pieces : -1]
    out_ref = refs[-1]
    width = q_ref.shape[1]
    rows = q_ref.shape[0]
    sizes = [ref.shape[1] for ref in kv_refs]
    if keyed:
        ids = mask_refs[0][...]
        biases = [
            jnp.where(ids == mask_refs[1][i], 0.0, NEGATIVE).astype(jnp.float32)
            for i in range(pieces)
        ]
    else:
        biases = [mask_refs[0][0, i] for i in range(pieces)]
    lane = lax.broadcasted_iota(jnp.int32, (rows, LANES), 1)
    for pair in range(width // LANES):
        cols = slice(pair * LANES, (pair + 1) * LANES)
        queries = q_ref[:, cols]
        halves = []
        for odd in range(LANES // HD):
            mine = (lane >= odd * HD) & (lane < (odd + 1) * HD)
            picked = jnp.where(mine, queries.astype(jnp.float32) * HD ** (-0.5), 0.0).astype(
                jnp.bfloat16
            )
            scores = [
                lax.dot_general(
                    picked,
                    kv_refs[i][0, :, cols],
                    (((1,), (1,)), ((), ())),
                    preferred_element_type=jnp.float32,
                )
                + biases[i]
                for i in range(pieces)
            ]
            top = functools.reduce(
                jnp.maximum, [jnp.max(part, axis=1, keepdims=True) for part in scores]
            )
            total = None
            for i in range(pieces):
                weights = jnp.exp(scores[i] - top).astype(jnp.bfloat16)
                values = jnp.concatenate(
                    [kv_refs[i][1, :, cols], jnp.ones((sizes[i], LANES), jnp.bfloat16)], axis=1
                )
                part = dot(weights, values)
                total = part if total is None else total + part
            halves.append((mine, total[:, :LANES] / total[:, LANES:]))
        merged = halves[0][1]
        for mine, half in halves[1:]:
            merged = jnp.where(mine, half, merged)
        out_ref[:, cols] = merged.astype(jnp.bfloat16)


def attend(queries, kv_list, masks, keyed):
    rows, width = queries.shape
    pieces = len(kv_list)
    whole = lambda value: pl.BlockSpec(value.shape, lambda i: (0,) * value.ndim)
    if keyed:
        mask_specs = [pl.BlockSpec((BLOCK, 1), lambda i: (i, 0)), whole(masks[1])]
    else:
        mask_specs = [pl.BlockSpec((1,) + masks[0].shape[1:], lambda i: (i, 0, 0, 0))]
    return pl.pallas_call(
        functools.partial(attention_kernel, pieces, keyed),
        grid=(rows // BLOCK,),
        in_specs=[pl.BlockSpec((BLOCK, width), lambda i: (i, 0))]
        + [whole(kv) for kv in kv_list]
        + mask_specs,
        out_specs=pl.BlockSpec((BLOCK, width), lambda i: (i, 0)),
        out_shape=jax.ShapeDtypeStruct((rows, width), jnp.bfloat16),
        compiler_params=pltpu.CompilerParams(dimension_semantics=("arbitrary",)),
    )(queries, *kv_list, *masks)


def list_bias(lists, counts, band_index, query_blocks, pool_blocks):
    mine = lax.dynamic_slice_in_dim(lists, band_index * query_blocks, query_blocks, 0)
    used = lax.dynamic_slice_in_dim(counts, band_index * query_blocks, query_blocks, 0)
    live = jnp.arange(lists.shape[1], dtype=jnp.int32)[None, :] < used[:, None]
    candidates = (band_index - 1) * pool_blocks + jnp.arange(3 * pool_blocks, dtype=jnp.int32)
    hit = (mine[:, :, None] == candidates[None, None, :]) & live[:, :, None]
    bias = jnp.where(jnp.any(hit, axis=1), 0.0, NEGATIVE).astype(jnp.float32)
    spread = jnp.broadcast_to(bias[:, :, None], bias.shape + (BLOCK,))
    return spread.reshape(query_blocks, 3, 1, pool_blocks * BLOCK)


def neighbours(block):
    count = lax.axis_size("band")
    forward = [(i, i + 1) for i in range(count - 1)]
    backward = [(target, source) for source, target in forward]
    return lax.ppermute(block, "band", forward), lax.ppermute(block, "band", backward)


def half_of(value, index):
    rows = value.shape[0] // 2
    return lax.dynamic_slice_in_dim(value, index * rows, rows, 0)


def head_sum_half(source, weight, side):
    away = dot(half_of(source, 1 - side), weight).astype(jnp.bfloat16)
    came = exchange(away, "head", 1)
    total = dot(half_of(source, side), weight).astype(jnp.bfloat16).astype(jnp.float32)
    total = total + came.astype(jnp.float32)
    bit = 2
    while bit < lax.axis_size("head"):
        sent = total.astype(jnp.bfloat16)
        total = sent.astype(jnp.float32) + exchange(sent, "head", bit).astype(jnp.float32)
        bit *= 2
    return total


def both_halves(half, side):
    other = exchange(half, "head", 1)
    low = jnp.where(side == 0, half, other)
    high = jnp.where(side == 0, other, half)
    return jnp.concatenate([low, high], axis=0)


def per_device(
    grid_feats,
    mesh_feats,
    enc_in,
    enc_out,
    proc_in,
    proc_out,
    ff_up,
    ff_down,
    dec_in,
    dec_out,
    enc_list,
    enc_count,
    dec_list,
    dec_count,
    window_ids,
):
    members = lax.axis_size("members")
    bands = lax.axis_size("band")
    heads = lax.axis_size("head")
    band_index = lax.axis_index("band")
    head_index = lax.axis_index("head")
    side = head_index % 2
    grid_rows = grid_feats.shape[0]
    mesh_rows = mesh_feats.shape[0]
    grid_blocks = grid_rows // BLOCK
    mesh_blocks = mesh_rows // BLOCK

    enc_w, enc_o = gather_projections(enc_in, enc_out)
    proc_w, proc_o = gather_projections(proc_in, proc_out)
    up = by_rows(gather(half_shard(ff_up, members)))
    down = by_columns(gather(half_shard(ff_down, members)))
    dec_w, dec_o = gather_projections(dec_in, dec_out)

    enc_bias = list_bias(enc_list, enc_count, band_index, mesh_blocks, grid_blocks)
    dec_bias = list_bias(dec_list, dec_count, band_index, grid_blocks, mesh_blocks)

    grid_norm = normed(grid_feats)
    mesh_norm = normed(mesh_feats)

    def project(source, weight):
        return dot(source, weight).astype(jnp.bfloat16)

    enc_kv = jnp.stack([project(grid_norm, enc_w[1]), project(grid_norm, enc_w[2])])
    low, high = neighbours(enc_kv)
    enc_q = project(mesh_norm, enc_w[0])
    enc_attn = attend(enc_q, [low, enc_kv, high], [enc_bias], False)
    state = half_of(mesh_feats, side).astype(jnp.float32) + head_sum_half(enc_attn, enc_o, side)

    proc_norm = both_halves(normed(state), side)
    pairs = jnp.stack([project(proc_norm, proc_w[1]), project(proc_norm, proc_w[2])])
    reach = (WINDOW + mesh_rows - 2) // mesh_rows
    if bands <= 2 * reach + 1:
        offsets = list(range(1, bands))
        routes = [[(i, (i - offset) % bands) for i in range(bands)] for offset in offsets]
    else:
        offsets = [sign * step for step in range(1, reach + 1) for sign in (1, -1)]
        routes = [
            [(i, i - offset) for i in range(bands) if 0 <= i - offset < bands]
            for offset in offsets
        ]
    slab = [pairs] + [lax.ppermute(pairs, "band", route) for route in routes]
    key_ids = []
    for offset in [0] + offsets:
        source = band_index + offset
        if bands <= 2 * reach + 1:
            source = source % bands
        inside = (source >= 0) & (source < bands)
        safe = jnp.clip(source, 0, bands - 1)
        ids = lax.dynamic_slice_in_dim(window_ids, safe * mesh_rows, mesh_rows, 0)
        key_ids.append(jnp.where(inside, ids, -1).reshape(1, mesh_rows))
    key_ids = jnp.stack(key_ids)
    query_ids = lax.dynamic_slice_in_dim(
        window_ids, band_index * mesh_rows, mesh_rows, 0
    ).reshape(mesh_rows, 1)
    proc_q = project(proc_norm, proc_w[0])
    proc_attn = attend(proc_q, slab, [query_ids, key_ids], True)
    state = state + head_sum_half(proc_attn, proc_o, side)

    ff_norm = both_halves(normed(state), side)
    hidden = jax.nn.gelu(dot(ff_norm, up), approximate=False).astype(jnp.bfloat16)
    state = state + head_sum_half(hidden, down, side)

    final_norm = both_halves(normed(state), side)
    dec_kv = jnp.stack([project(final_norm, dec_w[1]), project(final_norm, dec_w[2])])
    low, high = neighbours(dec_kv)
    dec_q = project(grid_norm, dec_w[0])
    dec_attn = attend(dec_q, [low, dec_kv, high], [dec_bias], False)

    share = grid_rows // heads
    rows_of = dec_attn.reshape(heads // 2, 2, share, dec_attn.shape[1])

    def side_product(which):
        picked = lax.dynamic_index_in_dim(rows_of, which, 1, keepdims=False)
        return dot(picked.reshape(-1, picked.shape[-1]), dec_o).astype(jnp.bfloat16)

    came = exchange(side_product(1 - side), "head", 1)
    total = side_product(side).astype(jnp.float32) + came.astype(jnp.float32)
    bit = 2
    position = head_index // 2
    while bit < heads:
        parts = total.reshape(-1, 2, share, total.shape[1])
        mine = position % 2
        send = lax.dynamic_index_in_dim(parts, 1 - mine, 1, keepdims=False)
        keep = lax.dynamic_index_in_dim(parts, mine, 1, keepdims=False)
        got = exchange(send.astype(jnp.bfloat16), "head", bit)
        total = (
            keep.astype(jnp.bfloat16).astype(jnp.float32) + got.astype(jnp.float32)
        ).reshape(-1, total.shape[1])
        position = position // 2
        bit *= 2
    residual = lax.dynamic_slice_in_dim(grid_feats, head_index * share, share, 0)
    return (residual.astype(jnp.float32) + total).astype(jnp.bfloat16)


def solution(mesh):
    return jax.shard_map(
        per_device,
        mesh=mesh,
        in_specs=(
            P(("members", "band"), None),
            P(("members", "band"), None),
            P(None, "band", "head"),
            P("head", "band"),
            P(None, "band", "head"),
            P("head", "band"),
            P("band", "head"),
            P("head", "band"),
            P(None, "band", "head"),
            P("head", "band"),
            P(),
            P(),
            P(),
            P(),
            P(),
        ),
        out_specs=P(("members", "band", "head"), None),
        check_vma=False,
    )
```

```python
import functools

import jax
import jax.numpy as jnp
from jax import lax
from jax.experimental import pallas as pl
from jax.experimental.pallas import tpu as pltpu
from jax.sharding import PartitionSpec as P


HD = 64
BLOCK = 128
WINDOW = 1536
LANES = 128

EPSILON = 1e-05
NEGATIVE = -1e30


def dot(a, b):
    return jnp.dot(a, b, preferred_element_type=jnp.float32)


def normed(values):
    values = values.astype(jnp.float32)
    centred = values - jnp.mean(values, axis=-1, keepdims=True)
    variance = jnp.mean(centred * centred, axis=-1, keepdims=True)
    return (centred * lax.rsqrt(variance + EPSILON)).astype(jnp.bfloat16)


def exchange(value, axis, bit):
    count = lax.axis_size(axis)
    return lax.ppermute(value, axis, [(i, i ^ bit) for i in range(count)])


def half_shard(weight, members):
    rows = weight.shape[0] // members
    return lax.dynamic_slice_in_dim(weight, lax.axis_index("members") * rows, rows, 0)


def gather(value):
    members, bands = lax.axis_size("members"), lax.axis_size("band")
    whole = lax.all_gather(value, ("members", "band"), axis=0, tiled=False)
    return whole.reshape((members, bands) + value.shape)


def by_rows(pieces):
    members, bands, rows, columns = pieces.shape
    return pieces.transpose(1, 0, 2, 3).reshape(bands * members * rows, columns)


def by_columns(pieces):
    members, bands, rows, columns = pieces.shape
    return pieces.transpose(0, 2, 1, 3).reshape(members * rows, bands * columns)


def gather_projections(w_in, w_out):
    members = lax.axis_size("members")
    k_rows = w_in.shape[1] // members
    o_rows = w_out.shape[0] // members
    member = lax.axis_index("members")
    part_in = lax.dynamic_slice_in_dim(w_in, member * k_rows, k_rows, 1)
    part_out = half_shard(w_out, members)
    width = w_in.shape[2]
    flat_in = part_in.reshape(3 * k_rows, width)
    flat_out = part_out.reshape(-1, width)
    pieces = gather(jnp.concatenate([flat_in, flat_out], axis=0))
    bands = pieces.shape[1]
    mats = [by_rows(pieces[:, :, i * k_rows : (i + 1) * k_rows]) for i in range(3)]
    outs = pieces[:, :, 3 * k_rows :].reshape(members, bands, o_rows, w_out.shape[1])
    return mats, by_columns(outs)


def attention_kernel(pieces, keyed, *refs):
    q_ref = refs[0]
    kv_refs = refs[1 : 1 + pieces]
    mask_refs = refs[1 + pieces : -1]
    out_ref = refs[-1]
    width = q_ref.shape[1]
    rows = q_ref.shape[0]
    sizes = [ref.shape[1] for ref in kv_refs]
    if keyed:
        ids = mask_refs[0][...]
        biases = [
            jnp.where(ids == mask_refs[1][i], 0.0, NEGATIVE).astype(jnp.float32)
            for i in range(pieces)
        ]
    else:
        biases = [mask_refs[0][0, i] for i in range(pieces)]
    lane = lax.broadcasted_iota(jnp.int32, (rows, LANES), 1)
    for pair in range(width // LANES):
        cols = slice(pair * LANES, (pair + 1) * LANES)
        queries = q_ref[:, cols]
        halves = []
        for odd in range(LANES // HD):
            mine = (lane >= odd * HD) & (lane < (odd + 1) * HD)
            picked = jnp.where(mine, queries.astype(jnp.float32) * HD ** (-0.5), 0.0).astype(
                jnp.bfloat16
            )
            scores = [
                lax.dot_general(
                    picked,
                    kv_refs[i][0, :, cols],
                    (((1,), (1,)), ((), ())),
                    preferred_element_type=jnp.float32,
                )
                + biases[i]
                for i in range(pieces)
            ]
            top = functools.reduce(
                jnp.maximum, [jnp.max(part, axis=1, keepdims=True) for part in scores]
            )
            total = None
            for i in range(pieces):
                weights = jnp.exp(scores[i] - top).astype(jnp.bfloat16)
                values = jnp.concatenate(
                    [kv_refs[i][1, :, cols], jnp.ones((sizes[i], LANES), jnp.bfloat16)], axis=1
                )
                part = dot(weights, values)
                total = part if total is None else total + part
            halves.append((mine, total[:, :LANES] / total[:, LANES:]))
        merged = halves[0][1]
        for mine, half in halves[1:]:
            merged = jnp.where(mine, half, merged)
        out_ref[:, cols] = merged.astype(jnp.bfloat16)


def attend(queries, kv_list, masks, keyed):
    rows, width = queries.shape
    pieces = len(kv_list)
    whole = lambda value: pl.BlockSpec(value.shape, lambda i: (0,) * value.ndim)
    if keyed:
        mask_specs = [pl.BlockSpec((BLOCK, 1), lambda i: (i, 0)), whole(masks[1])]
    else:
        mask_specs = [pl.BlockSpec((1,) + masks[0].shape[1:], lambda i: (i, 0, 0, 0))]
    return pl.pallas_call(
        functools.partial(attention_kernel, pieces, keyed),
        grid=(rows // BLOCK,),
        in_specs=[pl.BlockSpec((BLOCK, width), lambda i: (i, 0))]
        + [whole(kv) for kv in kv_list]
        + mask_specs,
        out_specs=pl.BlockSpec((BLOCK, width), lambda i: (i, 0)),
        out_shape=jax.ShapeDtypeStruct((rows, width), jnp.bfloat16),
        compiler_params=pltpu.CompilerParams(dimension_semantics=("arbitrary",)),
    )(queries, *kv_list, *masks)


def list_bias(lists, counts, band_index, query_blocks, pool_blocks):
    mine = lax.dynamic_slice_in_dim(lists, band_index * query_blocks, query_blocks, 0)
    used = lax.dynamic_slice_in_dim(counts, band_index * query_blocks, query_blocks, 0)
    live = jnp.arange(lists.shape[1], dtype=jnp.int32)[None, :] < used[:, None]
    candidates = (band_index - 1) * pool_blocks + jnp.arange(3 * pool_blocks, dtype=jnp.int32)
    hit = (mine[:, :, None] == candidates[None, None, :]) & live[:, :, None]
    bias = jnp.where(jnp.any(hit, axis=1), 0.0, NEGATIVE).astype(jnp.float32)
    spread = jnp.broadcast_to(bias[:, :, None], bias.shape + (BLOCK,))
    return spread.reshape(query_blocks, 3, 1, pool_blocks * BLOCK)


def neighbours(block):
    count = lax.axis_size("band")
    forward = [(i, i + 1) for i in range(count - 1)]
    backward = [(target, source) for source, target in forward]
    return lax.ppermute(block, "band", forward), lax.ppermute(block, "band", backward)


def half_of(value, index):
    rows = value.shape[0] // 2
    return lax.dynamic_slice_in_dim(value, index * rows, rows, 0)


def head_sum_half(source, weight, side):
    away = dot(half_of(source, 1 - side), weight).astype(jnp.bfloat16)
    came = exchange(away, "head", 1)
    total = dot(half_of(source, side), weight).astype(jnp.bfloat16).astype(jnp.float32)
    total = total + came.astype(jnp.float32)
    bit = 2
    while bit < lax.axis_size("head"):
        sent = total.astype(jnp.bfloat16)
        total = sent.astype(jnp.float32) + exchange(sent, "head", bit).astype(jnp.float32)
        bit *= 2
    return total


def both_halves(half, side):
    other = exchange(half, "head", 1)
    low = jnp.where(side == 0, half, other)
    high = jnp.where(side == 0, other, half)
    return jnp.concatenate([low, high], axis=0)


def per_device(
    grid_feats,
    mesh_feats,
    enc_in,
    enc_out,
    proc_in,
    proc_out,
    ff_up,
    ff_down,
    dec_in,
    dec_out,
    enc_list,
    enc_count,
    dec_list,
    dec_count,
    window_ids,
):
    members = lax.axis_size("members")
    bands = lax.axis_size("band")
    heads = lax.axis_size("head")
    band_index = lax.axis_index("band")
    head_index = lax.axis_index("head")
    side = head_index % 2
    grid_rows = grid_feats.shape[0]
    mesh_rows = mesh_feats.shape[0]
    grid_blocks = grid_rows // BLOCK
    mesh_blocks = mesh_rows // BLOCK

    enc_w, enc_o = gather_projections(enc_in, enc_out)
    proc_w, proc_o = gather_projections(proc_in, proc_out)
    up = by_rows(gather(half_shard(ff_up, members)))
    down = by_columns(gather(half_shard(ff_down, members)))
    dec_w, dec_o = gather_projections(dec_in, dec_out)

    enc_bias = list_bias(enc_list, enc_count, band_index, mesh_blocks, grid_blocks)
    dec_bias = list_bias(dec_list, dec_count, band_index, grid_blocks, mesh_blocks)

    grid_norm = normed(grid_feats)
    mesh_norm = normed(mesh_feats)

    def project(source, weight):
        return dot(source, weight).astype(jnp.bfloat16)

    enc_kv = jnp.stack([project(grid_norm, enc_w[1]), project(grid_norm, enc_w[2])])
    low, high = neighbours(enc_kv)
    enc_q = project(mesh_norm, enc_w[0])
    enc_attn = attend(enc_q, [low, enc_kv, high], [enc_bias], False)
    state = half_of(mesh_feats, side).astype(jnp.float32) + head_sum_half(enc_attn, enc_o, side)

    proc_norm = both_halves(normed(state), side)
    pairs = jnp.stack([project(proc_norm, proc_w[1]), project(proc_norm, proc_w[2])])
    reach = (WINDOW + mesh_rows - 2) // mesh_rows
    if bands <= 2 * reach + 1:
        offsets = list(range(1, bands))
        routes = [[(i, (i - offset) % bands) for i in range(bands)] for offset in offsets]
    else:
        offsets = [sign * step for step in range(1, reach + 1) for sign in (1, -1)]
        routes = [
            [(i, i - offset) for i in range(bands) if 0 <= i - offset < bands]
            for offset in offsets
        ]
    slab = [pairs] + [lax.ppermute(pairs, "band", route) for route in routes]
    key_ids = []
    for offset in [0] + offsets:
        source = band_index + offset
        if bands <= 2 * reach + 1:
            source = source % bands
        inside = (source >= 0) & (source < bands)
        safe = jnp.clip(source, 0, bands - 1)
        ids = lax.dynamic_slice_in_dim(window_ids, safe * mesh_rows, mesh_rows, 0)
        key_ids.append(jnp.where(inside, ids, -1).reshape(1, mesh_rows))
    key_ids = jnp.stack(key_ids)
    query_ids = lax.dynamic_slice_in_dim(
        window_ids, band_index * mesh_rows, mesh_rows, 0
    ).reshape(mesh_rows, 1)
    proc_q = project(proc_norm, proc_w[0])
    proc_attn = attend(proc_q, slab, [query_ids, key_ids], True)
    state = state + head_sum_half(proc_attn, proc_o, side)

    ff_norm = both_halves(normed(state), side)
    hidden = jax.nn.gelu(dot(ff_norm, up), approximate=False).astype(jnp.bfloat16)
    state = state + head_sum_half(hidden, down, side)

    final_norm = both_halves(normed(state), side)
    dec_kv = jnp.stack([project(final_norm, dec_w[1]), project(final_norm, dec_w[2])])
    low, high = neighbours(dec_kv)
    dec_q = project(grid_norm, dec_w[0])
    dec_attn = attend(dec_q, [low, dec_kv, high], [dec_bias], False)

    share = grid_rows // heads
    rows_of = dec_attn.reshape(heads // 2, 2, share, dec_attn.shape[1])

    def side_product(which):
        picked = lax.dynamic_index_in_dim(rows_of, which, 1, keepdims=False)
        return dot(picked.reshape(-1, picked.shape[-1]), dec_o).astype(jnp.bfloat16)

    came = exchange(side_product(1 - side), "head", 1)
    total = side_product(side).astype(jnp.float32) + came.astype(jnp.float32)
    bit = 2
    position = head_index // 2
    while bit < heads:
        parts = total.reshape(-1, 2, share, total.shape[1])
        mine = position % 2
        send = lax.dynamic_index_in_dim(parts, 1 - mine, 1, keepdims=False)
        keep = lax.dynamic_index_in_dim(parts, mine, 1, keepdims=False)
        got = exchange(send.astype(jnp.bfloat16), "head", bit)
        total = (
            keep.astype(jnp.bfloat16).astype(jnp.float32) + got.astype(jnp.float32)
        ).reshape(-1, total.shape[1])
        position = position // 2
        bit *= 2
    residual = lax.dynamic_slice_in_dim(grid_feats, head_index * share, share, 0)
    return (residual.astype(jnp.float32) + total).astype(jnp.bfloat16)


def own_half(weight, axis):
    size = weight.shape[axis] // 2
    return lax.dynamic_slice_in_dim(weight, lax.axis_index("members") * size, size, axis)


def swap(value):
    return lax.ppermute(value, "members", [(0, 1), (1, 0)])


def stacked_columns(weight):
    return jnp.concatenate(
        [weight[:, i : i + LANES] for i in range(0, weight.shape[1], LANES)], axis=0
    )


def pack(w_in, w_out, which):
    parts = {name: own_half(w_in[i], 1) for i, name in enumerate("qkv") if name in which}
    if "o" in which:
        parts["o"] = stacked_columns(own_half(w_out, 0))
    return jnp.concatenate([parts[name] for name in which], axis=1)


def band_gather(value):
    return lax.all_gather(value, "band", axis=0, tiled=True)


def project_kernel(widths, *refs):
    source, own, other = refs[:3]
    for (start, width), out in zip(widths, refs[3:]):
        for place, weight in enumerate((own, other)):
            out[:, place * width : (place + 1) * width] = dot(
                source[...], weight[:, start : start + width]
            ).astype(jnp.bfloat16)


def project_pair(source, own, other, widths):
    rows = source.shape[0]
    return pl.pallas_call(
        functools.partial(project_kernel, widths),
        out_shape=[jax.ShapeDtypeStruct((rows, 2 * w), jnp.bfloat16) for _, w in widths],
    )(source, own, other)


def pair_attention_kernel(pieces, keyed, o_start, order_ref, *refs):
    q_ref = refs[0]
    kv_refs = refs[1 : 1 + pieces]
    masks = 2 if keyed else 1
    mask_refs = refs[1 + pieces : 1 + pieces + masks]
    weight_refs = refs[1 + pieces + masks : 3 + pieces + masks]
    away_ref, keep_ref = refs[3 + pieces + masks :]
    rows = q_ref.shape[0]
    step = pl.program_id(0)
    half = pl.num_programs(0) // 2
    if keyed:
        ids = mask_refs[0][...]
        biases = [
            jnp.where(ids == mask_refs[1][i], 0.0, NEGATIVE).astype(jnp.float32)
            for i in range(pieces)
        ]
    else:
        biases = [mask_refs[0][0, i] for i in range(pieces)]
    lane = lax.broadcasted_iota(jnp.int32, (rows, LANES), 1)
    mixed = []
    for pair in range(2):
        queries = q_ref[:, pair * LANES : (pair + 1) * LANES]
        key_cols = slice(2 * pair * LANES, (2 * pair + 1) * LANES)
        value_cols = slice((2 * pair + 1) * LANES, (2 * pair + 2) * LANES)
        merged = None
        for odd in range(LANES // HD):
            mine = (lane >= odd * HD) & (lane < (odd + 1) * HD)
            picked = jnp.where(mine, queries.astype(jnp.float32) * HD ** (-0.5), 0.0).astype(
                jnp.bfloat16
            )
            scores = [
                lax.dot_general(
                    picked,
                    kv_refs[i][:, key_cols],
                    (((1,), (1,)), ((), ())),
                    preferred_element_type=jnp.float32,
                )
                + biases[i]
                for i in range(pieces)
            ]
            top = functools.reduce(
                jnp.maximum, [jnp.max(part, axis=1, keepdims=True) for part in scores]
            )
            total = None
            for i in range(pieces):
                weights = jnp.exp(scores[i] - top).astype(jnp.bfloat16)
                values = kv_refs[i][:, value_cols]
                values = jnp.concatenate([values, jnp.ones_like(values)], axis=1)
                part = dot(weights, values)
                total = part if total is None else total + part
            result = total[:, :LANES] / total[:, LANES:]
            merged = result if merged is None else jnp.where(mine, result, merged)
        mixed.append(merged.astype(jnp.bfloat16))

    def write(out_ref):
        for group in range(out_ref.shape[1] // LANES):
            cols = slice(group * LANES, (group + 1) * LANES)
            total = None
            for pair in range(2):
                part = dot(mixed[pair], weight_refs[pair][cols, o_start : o_start + LANES])
                total = part if total is None else total + part
            out_ref[:, cols] = total.astype(jnp.bfloat16)

    @pl.when(step < half)
    def _():
        write(away_ref)

    @pl.when(step >= half)
    def _():
        write(keep_ref)


def attend_pair(queries, kv_list, masks, keyed, weights, o_start, order):
    rows = queries.shape[0]
    blocks = rows // BLOCK
    features = weights[0].shape[0]
    pieces = len(kv_list)
    whole = lambda value: pl.BlockSpec(value.shape, lambda i, o: (0,) * value.ndim)
    if keyed:
        mask_specs = [pl.BlockSpec((BLOCK, 1), lambda i, o: (o[i], 0)), whole(masks[1])]
    else:
        mask_specs = [pl.BlockSpec((1,) + masks[0].shape[1:], lambda i, o: (o[i], 0, 0, 0))]
    half = blocks // 2
    out = jax.ShapeDtypeStruct((rows // 2, features), jnp.bfloat16)
    return pl.pallas_call(
        functools.partial(pair_attention_kernel, pieces, keyed, o_start),
        grid_spec=pltpu.PrefetchScalarGridSpec(
            num_scalar_prefetch=1,
            grid=(blocks,),
            in_specs=[pl.BlockSpec((BLOCK, queries.shape[1]), lambda i, o: (o[i], 0))]
            + [whole(kv) for kv in kv_list]
            + mask_specs
            + [whole(weight) for weight in weights],
            out_specs=[
                pl.BlockSpec((BLOCK, features), lambda i, o: (jnp.minimum(i, half - 1), 0)),
                pl.BlockSpec((BLOCK, features), lambda i, o: (jnp.maximum(i - half, 0), 0)),
            ],
        ),
        out_shape=[out, out],
        compiler_params=pltpu.CompilerParams(dimension_semantics=("arbitrary",)),
    )(order, queries, *kv_list, *masks, *weights)


def down_kernel(bands, order_ref, own_hidden, other_hidden, own, other, away_ref, keep_ref):
    step = pl.program_id(0)
    columns = own.shape[1]
    inner = own_hidden.shape[1]

    def write(out_ref):
        for band in range(bands):
            rows = slice(band * inner, (band + 1) * inner)
            out_ref[:, band * columns : (band + 1) * columns] = (
                dot(own_hidden[...], own[rows, :]) + dot(other_hidden[...], other[rows, :])
            ).astype(jnp.bfloat16)

    @pl.when(step == 0)
    def _():
        write(away_ref)

    @pl.when(step == 1)
    def _():
        write(keep_ref)


def down_pair(own_hidden, other_hidden, own, other, order):
    rows, inner = own_hidden.shape
    bands = own.shape[0] // inner
    features = bands * own.shape[1]
    whole = lambda value: pl.BlockSpec(value.shape, lambda i, o: (0,) * value.ndim)
    taken = pl.BlockSpec((rows // 2, inner), lambda i, o: (o[i], 0))
    placed = pl.BlockSpec((rows // 2, features), lambda i, o: (0, 0))
    out = jax.ShapeDtypeStruct((rows // 2, features), jnp.bfloat16)
    return pl.pallas_call(
        functools.partial(down_kernel, bands),
        grid_spec=pltpu.PrefetchScalarGridSpec(
            num_scalar_prefetch=1,
            grid=(2,),
            in_specs=[taken, taken, whole(own), whole(other)],
            out_specs=[placed, placed],
        ),
        out_shape=[out, out],
        compiler_params=pltpu.CompilerParams(dimension_semantics=("arbitrary",)),
    )(order, own_hidden, other_hidden, own, other)


def sum_over_head(away, keep):
    total = keep.astype(jnp.float32) + exchange(away, "head", 1).astype(jnp.float32)
    bit = 2
    while bit < lax.axis_size("head"):
        sent = total.astype(jnp.bfloat16)
        total = sent.astype(jnp.float32) + exchange(sent, "head", bit).astype(jnp.float32)
        bit *= 2
    return total


def slab_routes(bands, mesh_rows):
    reach = (WINDOW + mesh_rows - 2) // mesh_rows
    if bands <= 2 * reach + 1:
        offsets = list(range(1, bands))
        return True, offsets, [[(i, (i - o) % bands) for i in range(bands)] for o in offsets]
    offsets = [sign * step for step in range(1, reach + 1) for sign in (1, -1)]
    routes = [[(i, i - o) for i in range(bands) if 0 <= i - o < bands] for o in offsets]
    return False, offsets, routes


def slab_ids(window_ids, mesh_rows, offsets, around):
    bands = lax.axis_size("band")
    key_ids = []
    for offset in [0] + offsets:
        source = lax.axis_index("band") + offset
        if around:
            source = source % bands
        inside = (source >= 0) & (source < bands)
        safe = jnp.clip(source, 0, bands - 1)
        ids = lax.dynamic_slice_in_dim(window_ids, safe * mesh_rows, mesh_rows, 0)
        key_ids.append(jnp.where(inside, ids, -1).reshape(1, mesh_rows))
    query_ids = lax.dynamic_slice_in_dim(
        window_ids, lax.axis_index("band") * mesh_rows, mesh_rows, 0
    ).reshape(mesh_rows, 1)
    return query_ids, jnp.stack(key_ids)


def paired_device(
    grid_feats,
    mesh_feats,
    enc_in,
    enc_out,
    proc_in,
    proc_out,
    ff_up,
    ff_down,
    dec_in,
    dec_out,
    enc_list,
    enc_count,
    dec_list,
    dec_count,
    window_ids,
):
    bands = lax.axis_size("band")
    heads = lax.axis_size("head")
    band_index = lax.axis_index("band")
    head_index = lax.axis_index("head")
    side = head_index % 2
    grid_rows = grid_feats.shape[0]
    mesh_rows = mesh_feats.shape[0]
    grid_blocks = grid_rows // BLOCK
    mesh_blocks = mesh_rows // BLOCK
    half_blocks = mesh_blocks // 2
    turns = jnp.arange(mesh_blocks, dtype=jnp.int32)
    order = (turns + (1 - side) * half_blocks) % mesh_blocks
    sides = jnp.stack([1 - side, side]).astype(jnp.int32)
    barrier = lax.optimization_barrier
    kv_cols, q_cols = (0, 2 * LANES), (2 * LANES, LANES)
    o_start = 3 * LANES

    enc_kv_own = band_gather(pack(enc_in, enc_out, "kv"))
    enc_kv_other = swap(enc_kv_own)
    enc_qo_own = band_gather(barrier((pack(enc_in, enc_out, "qo"), enc_kv_own))[0])
    enc_qo_other = swap(enc_qo_own)
    packed = (
        pack(proc_in, proc_out, "kvqo"),
        own_half(ff_up, 1),
        own_half(ff_down, 0),
        pack(dec_in, dec_out, "kvqo"),
    )
    packed = barrier(packed + (enc_kv_own,))[:4]
    proc_own, up_own, down_own, dec_own = [band_gather(value) for value in packed]
    proc_other = swap(proc_own)
    up_other = swap(up_own)
    down_other = swap(down_own)
    dec_other = swap(dec_own)

    enc_bias = list_bias(enc_list, enc_count, band_index, mesh_blocks, grid_blocks)
    dec_bias = list_bias(dec_list, dec_count, band_index, grid_blocks, mesh_blocks)
    around, offsets, routes = slab_routes(bands, mesh_rows)
    query_ids, key_ids = slab_ids(window_ids, mesh_rows, offsets, around)

    grid_norm = normed(grid_feats)
    mesh_norm = normed(mesh_feats)

    (enc_kv,) = project_pair(grid_norm, enc_kv_own, enc_kv_other, [kv_cols])
    low, high = neighbours(enc_kv)
    (enc_q,) = project_pair(mesh_norm, enc_qo_own, enc_qo_other, [(0, LANES)])
    away, keep = attend_pair(
        enc_q, [low, enc_kv, high], [enc_bias], False, [enc_qo_own, enc_qo_other], LANES, order
    )
    state = half_of(mesh_feats, side).astype(jnp.float32) + sum_over_head(away, keep)

    proc_norm = both_halves(normed(state), side)
    proc_kv, proc_q = project_pair(proc_norm, proc_own, proc_other, [kv_cols, q_cols])
    slab = [proc_kv] + [lax.ppermute(proc_kv, "band", route) for route in routes]
    away, keep = attend_pair(
        proc_q, slab, [query_ids, key_ids], True, [proc_own, proc_other], o_start, order
    )
    state = state + sum_over_head(away, keep)

    ff_norm = both_halves(normed(state), side)
    hidden = [
        jax.nn.gelu(dot(ff_norm, up), approximate=False).astype(jnp.bfloat16)
        for up in (up_own, up_other)
    ]
    away, keep = down_pair(*hidden, down_own, down_other, sides)
    state = state + sum_over_head(away, keep)

    final_norm = both_halves(normed(state), side)
    (dec_q,) = project_pair(grid_norm, dec_own, dec_other, [q_cols])
    (dec_kv,) = project_pair(final_norm, dec_own, dec_other, [kv_cols])
    low, high = neighbours(dec_kv)
    share = grid_rows // heads
    by_core = turns.reshape(-1, 2, share // BLOCK).transpose(1, 0, 2).reshape(2, -1)
    dec_order = jnp.where(side == 0, by_core[::-1].reshape(-1), by_core.reshape(-1))
    away, keep = attend_pair(
        dec_q, [low, dec_kv, high], [dec_bias], False, [dec_own, dec_other], o_start, dec_order
    )
    total = keep.astype(jnp.float32) + exchange(away, "head", 1).astype(jnp.float32)
    bit = 2
    position = head_index // 2
    while bit < heads:
        parts = total.reshape(-1, 2, share, total.shape[1])
        mine = position % 2
        send = lax.dynamic_index_in_dim(parts, 1 - mine, 1, keepdims=False)
        kept = lax.dynamic_index_in_dim(parts, mine, 1, keepdims=False)
        got = exchange(send.astype(jnp.bfloat16), "head", bit)
        total = (
            kept.astype(jnp.bfloat16).astype(jnp.float32) + got.astype(jnp.float32)
        ).reshape(-1, total.shape[1])
        position = position // 2
        bit *= 2
    residual = lax.dynamic_slice_in_dim(grid_feats, head_index * share, share, 0)
    return (residual.astype(jnp.float32) + total).astype(jnp.bfloat16)


def body(*args):
    w_in, w_out = args[2], args[3]
    paired = (
        lax.axis_size("members") == 2
        and w_in.shape[2] == 4 * HD
        and 2 * HD == LANES
        and w_in.shape[1] == w_out.shape[1]
        and w_in.shape[1] % LANES == 0
        and args[0].shape[0] % (lax.axis_size("head") * BLOCK) == 0
        and args[0].shape[0] == args[1].shape[0]
    )
    if not paired:
        return per_device(*args)
    return paired_device(*args)


def solution(mesh):
    return jax.shard_map(
        body,
        mesh=mesh,
        in_specs=(
            P(("members", "band"), None),
            P(("members", "band"), None),
            P(None, "band", "head"),
            P("head", "band"),
            P(None, "band", "head"),
            P("head", "band"),
            P("band", "head"),
            P("head", "band"),
            P(None, "band", "head"),
            P("head", "band"),
            P(),
            P(),
            P(),
            P(),
            P(),
        ),
        out_specs=P(("members", "band", "head"), None),
        check_vma=False,
    )
```

```python
import functools

import jax
import jax.numpy as jnp
from jax import lax
from jax.experimental import pallas as pl
from jax.experimental.pallas import tpu as pltpu
from jax.sharding import PartitionSpec as P


HD = 64
BLOCK = 128
WINDOW = 1536
LANES = 128

EPSILON = 1e-05
NEGATIVE = -1e30


def dot(a, b):
    return jnp.dot(a, b, preferred_element_type=jnp.float32)


def normed(values):
    values = values.astype(jnp.float32)
    centred = values - jnp.mean(values, axis=-1, keepdims=True)
    variance = jnp.mean(centred * centred, axis=-1, keepdims=True)
    return (centred * lax.rsqrt(variance + EPSILON)).astype(jnp.bfloat16)


def exchange(value, axis, bit):
    count = lax.axis_size(axis)
    return lax.ppermute(value, axis, [(i, i ^ bit) for i in range(count)])


def half_shard(weight, members):
    rows = weight.shape[0] // members
    return lax.dynamic_slice_in_dim(weight, lax.axis_index("members") * rows, rows, 0)


def gather(value):
    members, bands = lax.axis_size("members"), lax.axis_size("band")
    whole = lax.all_gather(value, ("members", "band"), axis=0, tiled=False)
    return whole.reshape((members, bands) + value.shape)


def by_rows(pieces):
    members, bands, rows, columns = pieces.shape
    return pieces.transpose(1, 0, 2, 3).reshape(bands * members * rows, columns)


def by_columns(pieces):
    members, bands, rows, columns = pieces.shape
    return pieces.transpose(0, 2, 1, 3).reshape(members * rows, bands * columns)


def gather_projections(w_in, w_out):
    members = lax.axis_size("members")
    k_rows = w_in.shape[1] // members
    o_rows = w_out.shape[0] // members
    member = lax.axis_index("members")
    part_in = lax.dynamic_slice_in_dim(w_in, member * k_rows, k_rows, 1)
    part_out = half_shard(w_out, members)
    width = w_in.shape[2]
    flat_in = part_in.reshape(3 * k_rows, width)
    flat_out = part_out.reshape(-1, width)
    pieces = gather(jnp.concatenate([flat_in, flat_out], axis=0))
    bands = pieces.shape[1]
    mats = [by_rows(pieces[:, :, i * k_rows : (i + 1) * k_rows]) for i in range(3)]
    outs = pieces[:, :, 3 * k_rows :].reshape(members, bands, o_rows, w_out.shape[1])
    return mats, by_columns(outs)


def attention_kernel(pieces, keyed, *refs):
    q_ref = refs[0]
    kv_refs = refs[1 : 1 + pieces]
    mask_refs = refs[1 + pieces : -1]
    out_ref = refs[-1]
    width = q_ref.shape[1]
    rows = q_ref.shape[0]
    sizes = [ref.shape[1] for ref in kv_refs]
    if keyed:
        ids = mask_refs[0][...]
        biases = [
            jnp.where(ids == mask_refs[1][i], 0.0, NEGATIVE).astype(jnp.float32)
            for i in range(pieces)
        ]
    else:
        biases = [mask_refs[0][0, i] for i in range(pieces)]
    lane = lax.broadcasted_iota(jnp.int32, (rows, LANES), 1)
    for pair in range(width // LANES):
        cols = slice(pair * LANES, (pair + 1) * LANES)
        queries = q_ref[:, cols]
        halves = []
        for odd in range(LANES // HD):
            mine = (lane >= odd * HD) & (lane < (odd + 1) * HD)
            picked = jnp.where(mine, queries.astype(jnp.float32) * HD ** (-0.5), 0.0).astype(
                jnp.bfloat16
            )
            scores = [
                lax.dot_general(
                    picked,
                    kv_refs[i][0, :, cols],
                    (((1,), (1,)), ((), ())),
                    preferred_element_type=jnp.float32,
                )
                + biases[i]
                for i in range(pieces)
            ]
            top = functools.reduce(
                jnp.maximum, [jnp.max(part, axis=1, keepdims=True) for part in scores]
            )
            total = None
            for i in range(pieces):
                weights = jnp.exp(scores[i] - top).astype(jnp.bfloat16)
                values = jnp.concatenate(
                    [kv_refs[i][1, :, cols], jnp.ones((sizes[i], LANES), jnp.bfloat16)], axis=1
                )
                part = dot(weights, values)
                total = part if total is None else total + part
            halves.append((mine, total[:, :LANES] / total[:, LANES:]))
        merged = halves[0][1]
        for mine, half in halves[1:]:
            merged = jnp.where(mine, half, merged)
        out_ref[:, cols] = merged.astype(jnp.bfloat16)


def attend(queries, kv_list, masks, keyed):
    rows, width = queries.shape
    pieces = len(kv_list)
    whole = lambda value: pl.BlockSpec(value.shape, lambda i: (0,) * value.ndim)
    if keyed:
        mask_specs = [pl.BlockSpec((BLOCK, 1), lambda i: (i, 0)), whole(masks[1])]
    else:
        mask_specs = [pl.BlockSpec((1,) + masks[0].shape[1:], lambda i: (i, 0, 0, 0))]
    return pl.pallas_call(
        functools.partial(attention_kernel, pieces, keyed),
        grid=(rows // BLOCK,),
        in_specs=[pl.BlockSpec((BLOCK, width), lambda i: (i, 0))]
        + [whole(kv) for kv in kv_list]
        + mask_specs,
        out_specs=pl.BlockSpec((BLOCK, width), lambda i: (i, 0)),
        out_shape=jax.ShapeDtypeStruct((rows, width), jnp.bfloat16),
        compiler_params=pltpu.CompilerParams(dimension_semantics=("arbitrary",)),
    )(queries, *kv_list, *masks)


def list_bias(lists, counts, band_index, query_blocks, pool_blocks):
    mine = lax.dynamic_slice_in_dim(lists, band_index * query_blocks, query_blocks, 0)
    used = lax.dynamic_slice_in_dim(counts, band_index * query_blocks, query_blocks, 0)
    live = jnp.arange(lists.shape[1], dtype=jnp.int32)[None, :] < used[:, None]
    candidates = (band_index - 1) * pool_blocks + jnp.arange(3 * pool_blocks, dtype=jnp.int32)
    hit = (mine[:, :, None] == candidates[None, None, :]) & live[:, :, None]
    bias = jnp.where(jnp.any(hit, axis=1), 0.0, NEGATIVE).astype(jnp.float32)
    spread = jnp.broadcast_to(bias[:, :, None], bias.shape + (BLOCK,))
    return spread.reshape(query_blocks, 3, 1, pool_blocks * BLOCK)


def neighbours(block):
    count = lax.axis_size("band")
    forward = [(i, i + 1) for i in range(count - 1)]
    backward = [(target, source) for source, target in forward]
    return lax.ppermute(block, "band", forward), lax.ppermute(block, "band", backward)


def half_of(value, index):
    rows = value.shape[0] // 2
    return lax.dynamic_slice_in_dim(value, index * rows, rows, 0)


def head_sum_half(source, weight, side):
    away = dot(half_of(source, 1 - side), weight).astype(jnp.bfloat16)
    came = exchange(away, "head", 1)
    total = dot(half_of(source, side), weight).astype(jnp.bfloat16).astype(jnp.float32)
    total = total + came.astype(jnp.float32)
    bit = 2
    while bit < lax.axis_size("head"):
        sent = total.astype(jnp.bfloat16)
        total = sent.astype(jnp.float32) + exchange(sent, "head", bit).astype(jnp.float32)
        bit *= 2
    return total


def both_halves(half, side):
    other = exchange(half, "head", 1)
    low = jnp.where(side == 0, half, other)
    high = jnp.where(side == 0, other, half)
    return jnp.concatenate([low, high], axis=0)


def per_device(
    grid_feats,
    mesh_feats,
    enc_in,
    enc_out,
    proc_in,
    proc_out,
    ff_up,
    ff_down,
    dec_in,
    dec_out,
    enc_list,
    enc_count,
    dec_list,
    dec_count,
    window_ids,
):
    members = lax.axis_size("members")
    bands = lax.axis_size("band")
    heads = lax.axis_size("head")
    band_index = lax.axis_index("band")
    head_index = lax.axis_index("head")
    side = head_index % 2
    grid_rows = grid_feats.shape[0]
    mesh_rows = mesh_feats.shape[0]
    grid_blocks = grid_rows // BLOCK
    mesh_blocks = mesh_rows // BLOCK

    enc_w, enc_o = gather_projections(enc_in, enc_out)
    proc_w, proc_o = gather_projections(proc_in, proc_out)
    up = by_rows(gather(half_shard(ff_up, members)))
    down = by_columns(gather(half_shard(ff_down, members)))
    dec_w, dec_o = gather_projections(dec_in, dec_out)

    enc_bias = list_bias(enc_list, enc_count, band_index, mesh_blocks, grid_blocks)
    dec_bias = list_bias(dec_list, dec_count, band_index, grid_blocks, mesh_blocks)

    grid_norm = normed(grid_feats)
    mesh_norm = normed(mesh_feats)

    def project(source, weight):
        return dot(source, weight).astype(jnp.bfloat16)

    enc_kv = jnp.stack([project(grid_norm, enc_w[1]), project(grid_norm, enc_w[2])])
    low, high = neighbours(enc_kv)
    enc_q = project(mesh_norm, enc_w[0])
    enc_attn = attend(enc_q, [low, enc_kv, high], [enc_bias], False)
    state = half_of(mesh_feats, side).astype(jnp.float32) + head_sum_half(enc_attn, enc_o, side)

    proc_norm = both_halves(normed(state), side)
    pairs = jnp.stack([project(proc_norm, proc_w[1]), project(proc_norm, proc_w[2])])
    reach = (WINDOW + mesh_rows - 2) // mesh_rows
    if bands <= 2 * reach + 1:
        offsets = list(range(1, bands))
        routes = [[(i, (i - offset) % bands) for i in range(bands)] for offset in offsets]
    else:
        offsets = [sign * step for step in range(1, reach + 1) for sign in (1, -1)]
        routes = [
            [(i, i - offset) for i in range(bands) if 0 <= i - offset < bands]
            for offset in offsets
        ]
    slab = [pairs] + [lax.ppermute(pairs, "band", route) for route in routes]
    key_ids = []
    for offset in [0] + offsets:
        source = band_index + offset
        if bands <= 2 * reach + 1:
            source = source % bands
        inside = (source >= 0) & (source < bands)
        safe = jnp.clip(source, 0, bands - 1)
        ids = lax.dynamic_slice_in_dim(window_ids, safe * mesh_rows, mesh_rows, 0)
        key_ids.append(jnp.where(inside, ids, -1).reshape(1, mesh_rows))
    key_ids = jnp.stack(key_ids)
    query_ids = lax.dynamic_slice_in_dim(
        window_ids, band_index * mesh_rows, mesh_rows, 0
    ).reshape(mesh_rows, 1)
    proc_q = project(proc_norm, proc_w[0])
    proc_attn = attend(proc_q, slab, [query_ids, key_ids], True)
    state = state + head_sum_half(proc_attn, proc_o, side)

    ff_norm = both_halves(normed(state), side)
    hidden = jax.nn.gelu(dot(ff_norm, up), approximate=False).astype(jnp.bfloat16)
    state = state + head_sum_half(hidden, down, side)

    final_norm = both_halves(normed(state), side)
    dec_kv = jnp.stack([project(final_norm, dec_w[1]), project(final_norm, dec_w[2])])
    low, high = neighbours(dec_kv)
    dec_q = project(grid_norm, dec_w[0])
    dec_attn = attend(dec_q, [low, dec_kv, high], [dec_bias], False)

    share = grid_rows // heads
    rows_of = dec_attn.reshape(heads // 2, 2, share, dec_attn.shape[1])

    def side_product(which):
        picked = lax.dynamic_index_in_dim(rows_of, which, 1, keepdims=False)
        return dot(picked.reshape(-1, picked.shape[-1]), dec_o).astype(jnp.bfloat16)

    came = exchange(side_product(1 - side), "head", 1)
    total = side_product(side).astype(jnp.float32) + came.astype(jnp.float32)
    bit = 2
    position = head_index // 2
    while bit < heads:
        parts = total.reshape(-1, 2, share, total.shape[1])
        mine = position % 2
        send = lax.dynamic_index_in_dim(parts, 1 - mine, 1, keepdims=False)
        keep = lax.dynamic_index_in_dim(parts, mine, 1, keepdims=False)
        got = exchange(send.astype(jnp.bfloat16), "head", bit)
        total = (
            keep.astype(jnp.bfloat16).astype(jnp.float32) + got.astype(jnp.float32)
        ).reshape(-1, total.shape[1])
        position = position // 2
        bit *= 2
    residual = lax.dynamic_slice_in_dim(grid_feats, head_index * share, share, 0)
    return (residual.astype(jnp.float32) + total).astype(jnp.bfloat16)


def own_half(weight, axis):
    size = weight.shape[axis] // 2
    return lax.dynamic_slice_in_dim(weight, lax.axis_index("members") * size, size, axis)


def whole_pack(w_in, w_out, which, other):
    member = lax.axis_index("members")
    member = 1 - member if other else member
    take = lambda w, axis: lax.dynamic_slice_in_dim(
        w, member * (w.shape[axis] // 2), w.shape[axis] // 2, axis
    )
    parts = {name: take(w_in[i], 1) for i, name in enumerate("qkv") if name in which}
    if "o" in which:
        parts["o"] = stacked_columns(take(w_out, 0))
    return jnp.concatenate([parts[name] for name in which], axis=1)


def from_bands(value):
    bands = lax.axis_size("band")
    pieces = [value]
    for step in range(1, bands):
        pieces.append(lax.ppermute(value, "band", [(i, (i - step) % bands) for i in range(bands)]))
    return pieces


def placed_kernel(groups, widths, source_ref, *refs):
    values = refs[0]
    bands = source_ref.shape[0]
    pieces = refs[1 : 1 + groups * bands]
    outs = refs[1 + groups * bands :]
    out, mats = outs[0], outs[1:]
    for group in range(groups):
        mat = mats[group]
        for band in range(bands):
            piece = pieces[group * bands + band]
            rows = piece.shape[0]
            start = pl.multiple_of(source_ref[band] * rows, rows)
            mat[pl.ds(start, rows), :] = piece[...]
    for group in range(groups):
        out[:, group * widths : (group + 1) * widths] = dot(
            values[...], mats[group][:, :widths]
        ).astype(jnp.bfloat16)


def project_placed(values, groups, widths, emit):
    bands = lax.axis_size("band")
    sources = (lax.axis_index("band") + jnp.arange(bands, dtype=jnp.int32)) % bands
    rows = values.shape[0]
    mat = (bands * groups[0][0].shape[0], groups[0][0].shape[1])
    out = jax.ShapeDtypeStruct((rows, len(groups) * widths), jnp.bfloat16)
    vmem = lambda: pl.BlockSpec(memory_space=pltpu.VMEM)
    mats = [jax.ShapeDtypeStruct(mat, jnp.bfloat16)] * len(groups)
    return pl.pallas_call(
        functools.partial(placed_kernel, len(groups), widths),
        in_specs=[pl.BlockSpec(memory_space=pltpu.SMEM)]
        + [vmem() for _ in range(1 + bands * len(groups))],
        out_specs=[vmem()] + ([vmem() for _ in groups] if emit else []),
        out_shape=[out] + (mats if emit else []),
        scratch_shapes=[] if emit else [pltpu.VMEM(mat, jnp.bfloat16) for _ in groups],
    )(sources, values, *[piece for group in groups for piece in group])


def swap(value):
    return lax.ppermute(value, "members", [(0, 1), (1, 0)])


def stacked_columns(weight):
    return jnp.concatenate(
        [weight[:, i : i + LANES] for i in range(0, weight.shape[1], LANES)], axis=0
    )


def pack(w_in, w_out, which):
    parts = {name: own_half(w_in[i], 1) for i, name in enumerate("qkv") if name in which}
    if "o" in which:
        parts["o"] = stacked_columns(own_half(w_out, 0))
    return jnp.concatenate([parts[name] for name in which], axis=1)


def band_gather(value):
    return lax.all_gather(value, "band", axis=0, tiled=True)


def project_kernel(widths, *refs):
    source, own, other = refs[:3]
    for (start, width), out in zip(widths, refs[3:]):
        for place, weight in enumerate((own, other)):
            out[:, place * width : (place + 1) * width] = dot(
                source[...], weight[:, start : start + width]
            ).astype(jnp.bfloat16)


def project_pair(source, own, other, widths):
    rows = source.shape[0]
    return pl.pallas_call(
        functools.partial(project_kernel, widths),
        out_shape=[jax.ShapeDtypeStruct((rows, 2 * w), jnp.bfloat16) for _, w in widths],
    )(source, own, other)


def pair_attention_kernel(pieces, keyed, o_start, order_ref, *refs):
    q_ref = refs[0]
    kv_refs = refs[1 : 1 + pieces]
    masks = 2 if keyed else 1
    mask_refs = refs[1 + pieces : 1 + pieces + masks]
    weight_refs = refs[1 + pieces + masks : 3 + pieces + masks]
    away_ref, keep_ref = refs[3 + pieces + masks :]
    rows = q_ref.shape[0]
    step = pl.program_id(0)
    half = pl.num_programs(0) // 2
    if keyed:
        ids = mask_refs[0][...]
        biases = [
            jnp.where(ids == mask_refs[1][i], 0.0, NEGATIVE).astype(jnp.float32)
            for i in range(pieces)
        ]
    else:
        biases = [mask_refs[0][0, i] for i in range(pieces)]
    lane = lax.broadcasted_iota(jnp.int32, (rows, LANES), 1)
    mixed = []
    for pair in range(2):
        queries = q_ref[:, pair * LANES : (pair + 1) * LANES]
        key_cols = slice(2 * pair * LANES, (2 * pair + 1) * LANES)
        value_cols = slice((2 * pair + 1) * LANES, (2 * pair + 2) * LANES)
        merged = None
        for odd in range(LANES // HD):
            mine = (lane >= odd * HD) & (lane < (odd + 1) * HD)
            picked = jnp.where(mine, queries.astype(jnp.float32) * HD ** (-0.5), 0.0).astype(
                jnp.bfloat16
            )
            scores = [
                lax.dot_general(
                    picked,
                    kv_refs[i][:, key_cols],
                    (((1,), (1,)), ((), ())),
                    preferred_element_type=jnp.float32,
                )
                + biases[i]
                for i in range(pieces)
            ]
            top = functools.reduce(
                jnp.maximum, [jnp.max(part, axis=1, keepdims=True) for part in scores]
            )
            total = None
            for i in range(pieces):
                weights = jnp.exp(scores[i] - top).astype(jnp.bfloat16)
                values = kv_refs[i][:, value_cols]
                values = jnp.concatenate([values, jnp.ones_like(values)], axis=1)
                part = dot(weights, values)
                total = part if total is None else total + part
            result = total[:, :LANES] / total[:, LANES:]
            merged = result if merged is None else jnp.where(mine, result, merged)
        mixed.append(merged.astype(jnp.bfloat16))

    def write(out_ref):
        for group in range(out_ref.shape[1] // LANES):
            cols = slice(group * LANES, (group + 1) * LANES)
            total = None
            for pair in range(2):
                part = dot(mixed[pair], weight_refs[pair][cols, o_start : o_start + LANES])
                total = part if total is None else total + part
            out_ref[:, cols] = total.astype(jnp.bfloat16)

    @pl.when(step < half)
    def _():
        write(away_ref)

    @pl.when(step >= half)
    def _():
        write(keep_ref)


def attend_pair(queries, kv_list, masks, keyed, weights, o_start, order):
    rows = queries.shape[0]
    blocks = rows // BLOCK
    features = weights[0].shape[0]
    pieces = len(kv_list)
    whole = lambda value: pl.BlockSpec(value.shape, lambda i, o: (0,) * value.ndim)
    if keyed:
        mask_specs = [pl.BlockSpec((BLOCK, 1), lambda i, o: (o[i], 0)), whole(masks[1])]
    else:
        mask_specs = [pl.BlockSpec((1,) + masks[0].shape[1:], lambda i, o: (o[i], 0, 0, 0))]
    half = blocks // 2
    out = jax.ShapeDtypeStruct((rows // 2, features), jnp.bfloat16)
    return pl.pallas_call(
        functools.partial(pair_attention_kernel, pieces, keyed, o_start),
        grid_spec=pltpu.PrefetchScalarGridSpec(
            num_scalar_prefetch=1,
            grid=(blocks,),
            in_specs=[pl.BlockSpec((BLOCK, queries.shape[1]), lambda i, o: (o[i], 0))]
            + [whole(kv) for kv in kv_list]
            + mask_specs
            + [whole(weight) for weight in weights],
            out_specs=[
                pl.BlockSpec((BLOCK, features), lambda i, o: (jnp.minimum(i, half - 1), 0)),
                pl.BlockSpec((BLOCK, features), lambda i, o: (jnp.maximum(i - half, 0), 0)),
            ],
        ),
        out_shape=[out, out],
        compiler_params=pltpu.CompilerParams(dimension_semantics=("arbitrary",)),
    )(order, queries, *kv_list, *masks, *weights)


def down_kernel(bands, order_ref, own_hidden, other_hidden, own, other, away_ref, keep_ref):
    step = pl.program_id(0)
    columns = own.shape[1]
    inner = own_hidden.shape[1]

    def write(out_ref):
        for band in range(bands):
            rows = slice(band * inner, (band + 1) * inner)
            out_ref[:, band * columns : (band + 1) * columns] = (
                dot(own_hidden[...], own[rows, :]) + dot(other_hidden[...], other[rows, :])
            ).astype(jnp.bfloat16)

    @pl.when(step == 0)
    def _():
        write(away_ref)

    @pl.when(step == 1)
    def _():
        write(keep_ref)


def down_pair(own_hidden, other_hidden, own, other, order):
    rows, inner = own_hidden.shape
    bands = own.shape[0] // inner
    features = bands * own.shape[1]
    whole = lambda value: pl.BlockSpec(value.shape, lambda i, o: (0,) * value.ndim)
    taken = pl.BlockSpec((rows // 2, inner), lambda i, o: (o[i], 0))
    placed = pl.BlockSpec((rows // 2, features), lambda i, o: (0, 0))
    out = jax.ShapeDtypeStruct((rows // 2, features), jnp.bfloat16)
    return pl.pallas_call(
        functools.partial(down_kernel, bands),
        grid_spec=pltpu.PrefetchScalarGridSpec(
            num_scalar_prefetch=1,
            grid=(2,),
            in_specs=[taken, taken, whole(own), whole(other)],
            out_specs=[placed, placed],
        ),
        out_shape=[out, out],
        compiler_params=pltpu.CompilerParams(dimension_semantics=("arbitrary",)),
    )(order, own_hidden, other_hidden, own, other)


def sum_over_head(away, keep):
    came = exchange(away, "head", 1)
    total = keep.astype(jnp.float32) + came.astype(jnp.float32)
    bit = 2
    while bit < lax.axis_size("head"):
        sent = total.astype(jnp.bfloat16)
        total = sent.astype(jnp.float32) + exchange(sent, "head", bit).astype(jnp.float32)
        bit *= 2
    return total


def slab_routes(bands, mesh_rows):
    reach = (WINDOW + mesh_rows - 2) // mesh_rows
    if bands <= 2 * reach + 1:
        offsets = list(range(1, bands))
        return True, offsets, [[(i, (i - o) % bands) for i in range(bands)] for o in offsets]
    offsets = [sign * step for step in range(1, reach + 1) for sign in (1, -1)]
    routes = [[(i, i - o) for i in range(bands) if 0 <= i - o < bands] for o in offsets]
    return False, offsets, routes


def slab_ids(window_ids, mesh_rows, offsets, around):
    bands = lax.axis_size("band")
    key_ids = []
    for offset in [0] + offsets:
        source = lax.axis_index("band") + offset
        if around:
            source = source % bands
        inside = (source >= 0) & (source < bands)
        safe = jnp.clip(source, 0, bands - 1)
        ids = lax.dynamic_slice_in_dim(window_ids, safe * mesh_rows, mesh_rows, 0)
        key_ids.append(jnp.where(inside, ids, -1).reshape(1, mesh_rows))
    query_ids = lax.dynamic_slice_in_dim(
        window_ids, lax.axis_index("band") * mesh_rows, mesh_rows, 0
    ).reshape(mesh_rows, 1)
    return query_ids, jnp.stack(key_ids)


def paired_device(
    grid_feats,
    mesh_feats,
    enc_in,
    enc_out,
    proc_in,
    proc_out,
    ff_up,
    ff_down,
    dec_in,
    dec_out,
    enc_list,
    enc_count,
    dec_list,
    dec_count,
    window_ids,
):
    bands = lax.axis_size("band")
    heads = lax.axis_size("head")
    band_index = lax.axis_index("band")
    head_index = lax.axis_index("head")
    side = head_index % 2
    grid_rows = grid_feats.shape[0]
    mesh_rows = mesh_feats.shape[0]
    grid_blocks = grid_rows // BLOCK
    mesh_blocks = mesh_rows // BLOCK
    half_blocks = mesh_blocks // 2
    turns = jnp.arange(mesh_blocks, dtype=jnp.int32)
    order = (turns + (1 - side) * half_blocks) % mesh_blocks
    sides = jnp.stack([1 - side, side]).astype(jnp.int32)
    barrier = lax.optimization_barrier
    kv_cols, q_cols = (0, 2 * LANES), (2 * LANES, LANES)
    o_start = 3 * LANES

    enc_kv_pieces = from_bands(
        jnp.concatenate([whole_pack(enc_in, enc_out, "kv", o) for o in (False, True)], axis=1),
    )
    enc_qo_own = from_bands(whole_pack(enc_in, enc_out, "qo", False))
    enc_qo_other = [whole_pack(enc_in, enc_out, "qo", True)]
    for piece in enc_qo_own[1:]:
        enc_qo_other.append(swap(piece))
    early = barrier((pack(proc_in, proc_out, "kvqo"), own_half(ff_up, 1), *enc_kv_pieces[1:]))
    proc_own, up_own = [band_gather(value) for value in early[:2]]
    proc_other = swap(proc_own)
    up_other = swap(up_own)

    enc_bias = list_bias(enc_list, enc_count, band_index, mesh_blocks, grid_blocks)
    dec_bias = list_bias(dec_list, dec_count, band_index, grid_blocks, mesh_blocks)
    around, offsets, routes = slab_routes(bands, mesh_rows)
    query_ids, key_ids = slab_ids(window_ids, mesh_rows, offsets, around)

    grid_norm = normed(grid_feats)
    mesh_norm = normed(mesh_feats)

    (enc_kv,) = project_placed(grid_norm, [enc_kv_pieces], 4 * LANES, False)
    low, high = neighbours(enc_kv)
    enc_q, qo_own, qo_other = project_placed(
        mesh_norm, [enc_qo_own, enc_qo_other], LANES, True
    )
    away, keep = attend_pair(
        enc_q, [low, enc_kv, high], [enc_bias], False, [qo_own, qo_other], LANES, order
    )
    state = half_of(mesh_feats, side).astype(jnp.float32) + sum_over_head(away, keep)

    proc_norm = both_halves(normed(state), side)
    proc_kv, proc_q = project_pair(proc_norm, proc_own, proc_other, [kv_cols, q_cols])
    slab = [proc_kv] + [lax.ppermute(proc_kv, "band", route) for route in routes]
    late = barrier((own_half(ff_down, 0), pack(dec_in, dec_out, "kvqo"), *slab[1:]))
    down_own = band_gather(late[0])
    down_other = swap(down_own)
    dec_own = band_gather(late[1])
    dec_other = swap(dec_own)
    away, keep = attend_pair(
        proc_q, slab, [query_ids, key_ids], True, [proc_own, proc_other], o_start, order
    )
    state = state + sum_over_head(away, keep)

    ff_norm = both_halves(normed(state), side)
    hidden = [
        jax.nn.gelu(dot(ff_norm, up), approximate=False).astype(jnp.bfloat16)
        for up in (up_own, up_other)
    ]
    away, keep = down_pair(*hidden, down_own, down_other, sides)
    state = state + sum_over_head(away, keep)

    final_norm = both_halves(normed(state), side)
    (dec_q,) = project_pair(grid_norm, dec_own, dec_other, [q_cols])
    (dec_kv,) = project_pair(final_norm, dec_own, dec_other, [kv_cols])
    low, high = neighbours(dec_kv)
    share = grid_rows // heads
    by_core = turns.reshape(-1, 2, share // BLOCK).transpose(1, 0, 2).reshape(2, -1)
    dec_order = jnp.where(side == 0, by_core[::-1].reshape(-1), by_core.reshape(-1))
    away, keep = attend_pair(
        dec_q, [low, dec_kv, high], [dec_bias], False, [dec_own, dec_other], o_start, dec_order
    )
    total = keep.astype(jnp.float32) + exchange(away, "head", 1).astype(jnp.float32)
    bit = 2
    position = head_index // 2
    while bit < heads:
        parts = total.reshape(-1, 2, share, total.shape[1])
        mine = position % 2
        send = lax.dynamic_index_in_dim(parts, 1 - mine, 1, keepdims=False)
        kept = lax.dynamic_index_in_dim(parts, mine, 1, keepdims=False)
        got = exchange(send.astype(jnp.bfloat16), "head", bit)
        total = (
            kept.astype(jnp.bfloat16).astype(jnp.float32) + got.astype(jnp.float32)
        ).reshape(-1, total.shape[1])
        position = position // 2
        bit *= 2
    residual = lax.dynamic_slice_in_dim(grid_feats, head_index * share, share, 0)
    return (residual.astype(jnp.float32) + total).astype(jnp.bfloat16)


def body(*args):
    w_in, w_out = args[2], args[3]
    paired = (
        lax.axis_size("members") == 2
        and w_in.shape[2] == 4 * HD
        and 2 * HD == LANES
        and w_in.shape[1] == w_out.shape[1]
        and w_in.shape[1] % LANES == 0
        and args[0].shape[0] % (lax.axis_size("head") * BLOCK) == 0
        and args[0].shape[0] == args[1].shape[0]
    )
    if not paired:
        return per_device(*args)
    return paired_device(*args)


def solution(mesh):
    return jax.shard_map(
        body,
        mesh=mesh,
        in_specs=(
            P(("members", "band"), None),
            P(("members", "band"), None),
            P(None, "band", "head"),
            P("head", "band"),
            P(None, "band", "head"),
            P("head", "band"),
            P("band", "head"),
            P("head", "band"),
            P(None, "band", "head"),
            P("head", "band"),
            P(),
            P(),
            P(),
            P(),
            P(),
        ),
        out_specs=P(("members", "band", "head"), None),
        check_vma=False,
    )
```

```python
import functools

import jax
import jax.numpy as jnp
from jax import lax
from jax.experimental import pallas as pl
from jax.experimental.pallas import tpu as pltpu
from jax.sharding import PartitionSpec as P


HD = 64
BLOCK = 128
WINDOW = 1536
LANES = 128

EPSILON = 1e-05
NEGATIVE = -1e30


def dot(a, b):
    return jnp.dot(a, b, preferred_element_type=jnp.float32)


def normed(values):
    values = values.astype(jnp.float32)
    centred = values - jnp.mean(values, axis=-1, keepdims=True)
    variance = jnp.mean(centred * centred, axis=-1, keepdims=True)
    return (centred * lax.rsqrt(variance + EPSILON)).astype(jnp.bfloat16)


def gelu(values):
    return 0.5 * values * (1.0 + lax.erf(values * 2.0 ** (-0.5)))


def exchange(value, axis, bit):
    count = lax.axis_size(axis)
    return lax.ppermute(value, axis, [(i, i ^ bit) for i in range(count)])


def half_shard(weight, members):
    rows = weight.shape[0] // members
    return lax.dynamic_slice_in_dim(weight, lax.axis_index("members") * rows, rows, 0)


def gather(value):
    members, bands = lax.axis_size("members"), lax.axis_size("band")
    whole = lax.all_gather(value, ("members", "band"), axis=0, tiled=False)
    return whole.reshape((members, bands) + value.shape)


def by_rows(pieces):
    members, bands, rows, columns = pieces.shape
    return pieces.transpose(1, 0, 2, 3).reshape(bands * members * rows, columns)


def by_columns(pieces):
    members, bands, rows, columns = pieces.shape
    return pieces.transpose(0, 2, 1, 3).reshape(members * rows, bands * columns)


def gather_projections(w_in, w_out):
    members = lax.axis_size("members")
    k_rows = w_in.shape[1] // members
    o_rows = w_out.shape[0] // members
    member = lax.axis_index("members")
    part_in = lax.dynamic_slice_in_dim(w_in, member * k_rows, k_rows, 1)
    part_out = half_shard(w_out, members)
    width = w_in.shape[2]
    flat_in = part_in.reshape(3 * k_rows, width)
    flat_out = part_out.reshape(-1, width)
    pieces = gather(jnp.concatenate([flat_in, flat_out], axis=0))
    bands = pieces.shape[1]
    mats = [by_rows(pieces[:, :, i * k_rows : (i + 1) * k_rows]) for i in range(3)]
    outs = pieces[:, :, 3 * k_rows :].reshape(members, bands, o_rows, w_out.shape[1])
    return mats, by_columns(outs)


def attention_kernel(pieces, keyed, *refs):
    q_ref = refs[0]
    kv_refs = refs[1 : 1 + pieces]
    mask_refs = refs[1 + pieces : -1]
    out_ref = refs[-1]
    width = q_ref.shape[1]
    rows = q_ref.shape[0]
    sizes = [ref.shape[1] for ref in kv_refs]
    if keyed:
        ids = mask_refs[0][...]
        biases = [
            jnp.where(ids == mask_refs[1][i], 0.0, NEGATIVE).astype(jnp.float32)
            for i in range(pieces)
        ]
    else:
        biases = [mask_refs[0][0, i] for i in range(pieces)]
    lane = lax.broadcasted_iota(jnp.int32, (rows, LANES), 1)
    for pair in range(width // LANES):
        cols = slice(pair * LANES, (pair + 1) * LANES)
        queries = q_ref[:, cols]
        halves = []
        for odd in range(LANES // HD):
            mine = (lane >= odd * HD) & (lane < (odd + 1) * HD)
            picked = jnp.where(mine, queries.astype(jnp.float32) * HD ** (-0.5), 0.0).astype(
                jnp.bfloat16
            )
            scores = [
                lax.dot_general(
                    picked,
                    kv_refs[i][0, :, cols],
                    (((1,), (1,)), ((), ())),
                    preferred_element_type=jnp.float32,
                )
                + biases[i]
                for i in range(pieces)
            ]
            top = functools.reduce(
                jnp.maximum, [jnp.max(part, axis=1, keepdims=True) for part in scores]
            )
            total = None
            for i in range(pieces):
                weights = jnp.exp(scores[i] - top).astype(jnp.bfloat16)
                values = jnp.concatenate(
                    [kv_refs[i][1, :, cols], jnp.ones((sizes[i], LANES), jnp.bfloat16)], axis=1
                )
                part = dot(weights, values)
                total = part if total is None else total + part
            halves.append((mine, total[:, :LANES] / total[:, LANES:]))
        merged = halves[0][1]
        for mine, half in halves[1:]:
            merged = jnp.where(mine, half, merged)
        out_ref[:, cols] = merged.astype(jnp.bfloat16)


def attend(queries, kv_list, masks, keyed):
    rows, width = queries.shape
    pieces = len(kv_list)
    whole = lambda value: pl.BlockSpec(value.shape, lambda i: (0,) * value.ndim)
    if keyed:
        mask_specs = [pl.BlockSpec((BLOCK, 1), lambda i: (i, 0)), whole(masks[1])]
    else:
        mask_specs = [pl.BlockSpec((1,) + masks[0].shape[1:], lambda i: (i, 0, 0, 0))]
    return pl.pallas_call(
        functools.partial(attention_kernel, pieces, keyed),
        grid=(rows // BLOCK,),
        in_specs=[pl.BlockSpec((BLOCK, width), lambda i: (i, 0))]
        + [whole(kv) for kv in kv_list]
        + mask_specs,
        out_specs=pl.BlockSpec((BLOCK, width), lambda i: (i, 0)),
        out_shape=jax.ShapeDtypeStruct((rows, width), jnp.bfloat16),
        compiler_params=pltpu.CompilerParams(dimension_semantics=("arbitrary",)),
    )(queries, *kv_list, *masks)


def list_bias(lists, counts, band_index, query_blocks, pool_blocks):
    mine = lax.dynamic_slice_in_dim(lists, band_index * query_blocks, query_blocks, 0)
    used = lax.dynamic_slice_in_dim(counts, band_index * query_blocks, query_blocks, 0)
    live = jnp.arange(lists.shape[1], dtype=jnp.int32)[None, :] < used[:, None]
    candidates = (band_index - 1) * pool_blocks + jnp.arange(3 * pool_blocks, dtype=jnp.int32)
    hit = (mine[:, :, None] == candidates[None, None, :]) & live[:, :, None]
    bias = jnp.where(jnp.any(hit, axis=1), 0.0, NEGATIVE).astype(jnp.float32)
    spread = jnp.broadcast_to(bias[:, :, None], bias.shape + (BLOCK,))
    return spread.reshape(query_blocks, 3, 1, pool_blocks * BLOCK)


def neighbours(block):
    count = lax.axis_size("band")
    forward = [(i, i + 1) for i in range(count - 1)]
    backward = [(target, source) for source, target in forward]
    return lax.ppermute(block, "band", forward), lax.ppermute(block, "band", backward)


def half_of(value, index):
    rows = value.shape[0] // 2
    return lax.dynamic_slice_in_dim(value, index * rows, rows, 0)


def head_sum_half(source, weight, side):
    away = dot(half_of(source, 1 - side), weight).astype(jnp.bfloat16)
    came = exchange(away, "head", 1)
    total = dot(half_of(source, side), weight).astype(jnp.bfloat16).astype(jnp.float32)
    total = total + came.astype(jnp.float32)
    bit = 2
    while bit < lax.axis_size("head"):
        sent = total.astype(jnp.bfloat16)
        total = sent.astype(jnp.float32) + exchange(sent, "head", bit).astype(jnp.float32)
        bit *= 2
    return total


def both_halves(half, side):
    other = exchange(half, "head", 1)
    low = jnp.where(side == 0, half, other)
    high = jnp.where(side == 0, other, half)
    return jnp.concatenate([low, high], axis=0)


def per_device(
    grid_feats,
    mesh_feats,
    enc_in,
    enc_out,
    proc_in,
    proc_out,
    ff_up,
    ff_down,
    dec_in,
    dec_out,
    enc_list,
    enc_count,
    dec_list,
    dec_count,
    window_ids,
):
    members = lax.axis_size("members")
    bands = lax.axis_size("band")
    heads = lax.axis_size("head")
    band_index = lax.axis_index("band")
    head_index = lax.axis_index("head")
    side = head_index % 2
    grid_rows = grid_feats.shape[0]
    mesh_rows = mesh_feats.shape[0]
    grid_blocks = grid_rows // BLOCK
    mesh_blocks = mesh_rows // BLOCK

    enc_w, enc_o = gather_projections(enc_in, enc_out)
    proc_w, proc_o = gather_projections(proc_in, proc_out)
    up = by_rows(gather(half_shard(ff_up, members)))
    down = by_columns(gather(half_shard(ff_down, members)))
    dec_w, dec_o = gather_projections(dec_in, dec_out)

    enc_bias = list_bias(enc_list, enc_count, band_index, mesh_blocks, grid_blocks)
    dec_bias = list_bias(dec_list, dec_count, band_index, grid_blocks, mesh_blocks)

    grid_norm = normed(grid_feats)
    mesh_norm = normed(mesh_feats)

    def project(source, weight):
        return dot(source, weight).astype(jnp.bfloat16)

    enc_kv = jnp.stack([project(grid_norm, enc_w[1]), project(grid_norm, enc_w[2])])
    low, high = neighbours(enc_kv)
    enc_q = project(mesh_norm, enc_w[0])
    enc_attn = attend(enc_q, [low, enc_kv, high], [enc_bias], False)
    state = half_of(mesh_feats, side).astype(jnp.float32) + head_sum_half(enc_attn, enc_o, side)

    proc_norm = both_halves(normed(state), side)
    pairs = jnp.stack([project(proc_norm, proc_w[1]), project(proc_norm, proc_w[2])])
    reach = (WINDOW + mesh_rows - 2) // mesh_rows
    if bands <= 2 * reach + 1:
        offsets = list(range(1, bands))
        routes = [[(i, (i - offset) % bands) for i in range(bands)] for offset in offsets]
    else:
        offsets = [sign * step for step in range(1, reach + 1) for sign in (1, -1)]
        routes = [
            [(i, i - offset) for i in range(bands) if 0 <= i - offset < bands]
            for offset in offsets
        ]
    slab = [pairs] + [lax.ppermute(pairs, "band", route) for route in routes]
    key_ids = []
    for offset in [0] + offsets:
        source = band_index + offset
        if bands <= 2 * reach + 1:
            source = source % bands
        inside = (source >= 0) & (source < bands)
        safe = jnp.clip(source, 0, bands - 1)
        ids = lax.dynamic_slice_in_dim(window_ids, safe * mesh_rows, mesh_rows, 0)
        key_ids.append(jnp.where(inside, ids, -1).reshape(1, mesh_rows))
    key_ids = jnp.stack(key_ids)
    query_ids = lax.dynamic_slice_in_dim(
        window_ids, band_index * mesh_rows, mesh_rows, 0
    ).reshape(mesh_rows, 1)
    proc_q = project(proc_norm, proc_w[0])
    proc_attn = attend(proc_q, slab, [query_ids, key_ids], True)
    state = state + head_sum_half(proc_attn, proc_o, side)

    ff_norm = both_halves(normed(state), side)
    hidden = jax.nn.gelu(dot(ff_norm, up), approximate=False).astype(jnp.bfloat16)
    state = state + head_sum_half(hidden, down, side)

    final_norm = both_halves(normed(state), side)
    dec_kv = jnp.stack([project(final_norm, dec_w[1]), project(final_norm, dec_w[2])])
    low, high = neighbours(dec_kv)
    dec_q = project(grid_norm, dec_w[0])
    dec_attn = attend(dec_q, [low, dec_kv, high], [dec_bias], False)

    share = grid_rows // heads
    rows_of = dec_attn.reshape(heads // 2, 2, share, dec_attn.shape[1])

    def side_product(which):
        picked = lax.dynamic_index_in_dim(rows_of, which, 1, keepdims=False)
        return dot(picked.reshape(-1, picked.shape[-1]), dec_o).astype(jnp.bfloat16)

    came = exchange(side_product(1 - side), "head", 1)
    total = side_product(side).astype(jnp.float32) + came.astype(jnp.float32)
    bit = 2
    position = head_index // 2
    while bit < heads:
        parts = total.reshape(-1, 2, share, total.shape[1])
        mine = position % 2
        send = lax.dynamic_index_in_dim(parts, 1 - mine, 1, keepdims=False)
        keep = lax.dynamic_index_in_dim(parts, mine, 1, keepdims=False)
        got = exchange(send.astype(jnp.bfloat16), "head", bit)
        total = (
            keep.astype(jnp.bfloat16).astype(jnp.float32) + got.astype(jnp.float32)
        ).reshape(-1, total.shape[1])
        position = position // 2
        bit *= 2
    residual = lax.dynamic_slice_in_dim(grid_feats, head_index * share, share, 0)
    return (residual.astype(jnp.float32) + total).astype(jnp.bfloat16)


def own_half(weight, axis):
    size = weight.shape[axis] // 2
    return lax.dynamic_slice_in_dim(weight, lax.axis_index("members") * size, size, axis)


def whole_pack(w_in, w_out, which, other):
    member = lax.axis_index("members")
    member = 1 - member if other else member
    take = lambda w, axis: lax.dynamic_slice_in_dim(
        w, member * (w.shape[axis] // 2), w.shape[axis] // 2, axis
    )
    parts = {name: take(w_in[i], 1) for i, name in enumerate("qkv") if name in which}
    if "o" in which:
        parts["o"] = stacked_columns(take(w_out, 0))
    return jnp.concatenate([parts[name] for name in which], axis=1)


def from_bands(value):
    bands = lax.axis_size("band")
    pieces = [value]
    for step in range(1, bands):
        pieces.append(lax.ppermute(value, "band", [(i, (i - step) % bands) for i in range(bands)]))
    return pieces


def placed_kernel(groups, widths, source_ref, *refs):
    values = refs[0]
    bands = source_ref.shape[0]
    pieces = refs[1 : 1 + groups * bands]
    outs = refs[1 + groups * bands :]
    out, mats = outs[0], outs[1:]
    for group in range(groups):
        mat = mats[group]
        for band in range(bands):
            piece = pieces[group * bands + band]
            rows = piece.shape[0]
            start = pl.multiple_of(source_ref[band] * rows, rows)
            mat[pl.ds(start, rows), :] = piece[...]
    for group in range(groups):
        out[:, group * widths : (group + 1) * widths] = dot(
            values[...], mats[group][:, :widths]
        ).astype(jnp.bfloat16)


def project_placed(values, groups, widths, emit):
    bands = lax.axis_size("band")
    sources = (lax.axis_index("band") + jnp.arange(bands, dtype=jnp.int32)) % bands
    rows = values.shape[0]
    mat = (bands * groups[0][0].shape[0], groups[0][0].shape[1])
    out = jax.ShapeDtypeStruct((rows, len(groups) * widths), jnp.bfloat16)
    vmem = lambda: pl.BlockSpec(memory_space=pltpu.VMEM)
    mats = [jax.ShapeDtypeStruct(mat, jnp.bfloat16)] * len(groups)
    return pl.pallas_call(
        functools.partial(placed_kernel, len(groups), widths),
        in_specs=[pl.BlockSpec(memory_space=pltpu.SMEM)]
        + [vmem() for _ in range(1 + bands * len(groups))],
        out_specs=[vmem()] + ([vmem() for _ in groups] if emit else []),
        out_shape=[out] + (mats if emit else []),
        scratch_shapes=[] if emit else [pltpu.VMEM(mat, jnp.bfloat16) for _ in groups],
    )(sources, values, *[piece for group in groups for piece in group])


def swap(value):
    return lax.ppermute(value, "members", [(0, 1), (1, 0)])


def stacked_columns(weight):
    return jnp.concatenate(
        [weight[:, i : i + LANES] for i in range(0, weight.shape[1], LANES)], axis=0
    )


def pack(w_in, w_out, which):
    parts = {name: own_half(w_in[i], 1) for i, name in enumerate("qkv") if name in which}
    if "o" in which:
        parts["o"] = stacked_columns(own_half(w_out, 0))
    return jnp.concatenate([parts[name] for name in which], axis=1)


def band_gather(value):
    return lax.all_gather(value, "band", axis=0, tiled=True)


def project_kernel(widths, side_ref, *refs):
    mine, theirs, own, other = refs[:4]
    rows = mine.shape[0]
    for half, place in ((mine, side_ref[0]), (theirs, 1 - side_ref[0])):
        start = pl.multiple_of(place * rows, rows)
        for (first, width), out in zip(widths, refs[4:]):
            for group, weight in enumerate((own, other)):
                out[pl.ds(start, rows), group * width : (group + 1) * width] = dot(
                    half[...], weight[:, first : first + width]
                ).astype(jnp.bfloat16)


def project_pair(mine, theirs, side, own, other, widths):
    rows = 2 * mine.shape[0]
    vmem = lambda: pl.BlockSpec(memory_space=pltpu.VMEM)
    return pl.pallas_call(
        functools.partial(project_kernel, widths),
        in_specs=[pl.BlockSpec(memory_space=pltpu.SMEM)] + [vmem() for _ in range(4)],
        out_specs=[vmem() for _ in widths],
        out_shape=[jax.ShapeDtypeStruct((rows, 2 * w), jnp.bfloat16) for _, w in widths],
    )(side.reshape(1).astype(jnp.int32), mine, theirs, own, other)


def pair_attention_kernel(pieces, keyed, o_start, order_ref, *refs):
    q_refs = refs[:2]
    kv_refs = refs[2 : 2 + pieces]
    mask_refs = refs[2 + pieces : 4 + pieces]
    rest = refs[4 + pieces :]
    if keyed:
        key_ids, rest = rest[0], rest[1:]
    weight_refs = rest[:2]
    away_ref, keep_ref = rest[2:]
    block = q_refs[0].shape[0]
    rows = 2 * block
    lane = lax.broadcasted_iota(jnp.int32, (rows, LANES), 1)

    def biased(scores, piece):
        parts = []
        for place in range(2):
            part = scores[place * block : (place + 1) * block]
            if keyed:
                part = jnp.where(mask_refs[place][...] == key_ids[piece], part, NEGATIVE)
            else:
                part = part + mask_refs[place][0, piece]
            parts.append(part)
        return jnp.concatenate(parts, axis=0)

    mixed = []
    for pair in range(2):
        cols = slice(pair * LANES, (pair + 1) * LANES)
        queries = jnp.concatenate([q_refs[0][:, cols], q_refs[1][:, cols]], axis=0)
        queries = queries.astype(jnp.float32) * HD ** (-0.5)
        key_cols = slice(2 * pair * LANES, (2 * pair + 1) * LANES)
        value_cols = slice((2 * pair + 1) * LANES, (2 * pair + 2) * LANES)
        merged = None
        for odd in range(LANES // HD):
            mine = (lane >= odd * HD) & (lane < (odd + 1) * HD)
            picked = jnp.where(mine, queries, 0.0).astype(jnp.bfloat16)
            scores = [
                biased(
                    lax.dot_general(
                        picked,
                        kv_refs[i][:, key_cols],
                        (((1,), (1,)), ((), ())),
                        preferred_element_type=jnp.float32,
                    ),
                    i,
                )
                for i in range(pieces)
            ]
            top = functools.reduce(
                jnp.maximum, [jnp.max(part, axis=1, keepdims=True) for part in scores]
            )
            total = None
            for i in range(pieces):
                weights = jnp.exp(scores[i] - top).astype(jnp.bfloat16)
                values = kv_refs[i][:, value_cols]
                values = jnp.concatenate([values, jnp.ones_like(values)], axis=1)
                part = dot(weights, values)
                total = part if total is None else total + part
            result = total[:, :LANES] / total[:, LANES:]
            merged = result if merged is None else jnp.where(mine, result, merged)
        mixed.append(merged.astype(jnp.bfloat16))

    def write(out_ref):
        for group in range(out_ref.shape[1] // LANES):
            cols = slice(group * LANES, (group + 1) * LANES)
            total = None
            for pair in range(2):
                part = dot(mixed[pair], weight_refs[pair][cols, o_start : o_start + LANES])
                total = part if total is None else total + part
            out_ref[:, cols] = total.astype(jnp.bfloat16)

    half = pl.num_programs(0) // 2

    @pl.when(pl.program_id(0) < half)
    def _():
        write(away_ref)

    @pl.when(pl.program_id(0) >= half)
    def _():
        write(keep_ref)


def attend_pair(queries, kv_list, masks, keyed, weights, o_start, order):
    rows = queries.shape[0]
    steps = rows // (2 * BLOCK)
    features = weights[0].shape[0]
    pieces = len(kv_list)
    whole = lambda value: pl.BlockSpec(value.shape, lambda i, o: (0,) * value.ndim)
    width = queries.shape[1]
    q_specs = [
        pl.BlockSpec((BLOCK, width), lambda i, o: (o[2 * i], 0)),
        pl.BlockSpec((BLOCK, width), lambda i, o: (o[2 * i + 1], 0)),
    ]
    if keyed:
        mask_specs = [
            pl.BlockSpec((BLOCK, 1), lambda i, o: (o[2 * i], 0)),
            pl.BlockSpec((BLOCK, 1), lambda i, o: (o[2 * i + 1], 0)),
            whole(masks[1]),
        ]
        masks = [masks[0], masks[0], masks[1]]
    else:
        block = (1,) + masks[0].shape[1:]
        mask_specs = [
            pl.BlockSpec(block, lambda i, o: (o[2 * i], 0, 0, 0)),
            pl.BlockSpec(block, lambda i, o: (o[2 * i + 1], 0, 0, 0)),
        ]
        masks = [masks[0], masks[0]]
    half = steps // 2
    out = jax.ShapeDtypeStruct((rows // 2, features), jnp.bfloat16)
    placed = (2 * BLOCK, features)
    return pl.pallas_call(
        functools.partial(pair_attention_kernel, pieces, keyed, o_start),
        grid_spec=pltpu.PrefetchScalarGridSpec(
            num_scalar_prefetch=1,
            grid=(steps,),
            in_specs=q_specs
            + [whole(kv) for kv in kv_list]
            + mask_specs
            + [whole(weight) for weight in weights],
            out_specs=[
                pl.BlockSpec(placed, lambda i, o: (jnp.minimum(i, half - 1), 0)),
                pl.BlockSpec(placed, lambda i, o: (jnp.maximum(i - half, 0), 0)),
            ],
        ),
        out_shape=[out, out],
        compiler_params=pltpu.CompilerParams(dimension_semantics=("arbitrary",)),
    )(order, queries, queries, *kv_list, *masks, *weights)


def down_kernel(bands, order_ref, own_hidden, other_hidden, own, other, away_ref, keep_ref):
    step = pl.program_id(0)
    columns = own.shape[1]
    inner = own_hidden.shape[1]

    def write(out_ref):
        for band in range(bands):
            rows = slice(band * inner, (band + 1) * inner)
            out_ref[:, band * columns : (band + 1) * columns] = (
                dot(own_hidden[...], own[rows, :]) + dot(other_hidden[...], other[rows, :])
            ).astype(jnp.bfloat16)

    @pl.when(step == 0)
    def _():
        write(away_ref)

    @pl.when(step == 1)
    def _():
        write(keep_ref)


def down_pair(own_hidden, other_hidden, own, other, order):
    rows, inner = own_hidden.shape
    bands = own.shape[0] // inner
    features = bands * own.shape[1]
    whole = lambda value: pl.BlockSpec(value.shape, lambda i, o: (0,) * value.ndim)
    taken = pl.BlockSpec((rows // 2, inner), lambda i, o: (o[i], 0))
    placed = pl.BlockSpec((rows // 2, features), lambda i, o: (0, 0))
    out = jax.ShapeDtypeStruct((rows // 2, features), jnp.bfloat16)
    return pl.pallas_call(
        functools.partial(down_kernel, bands),
        grid_spec=pltpu.PrefetchScalarGridSpec(
            num_scalar_prefetch=1,
            grid=(2,),
            in_specs=[taken, taken, whole(own), whole(other)],
            out_specs=[placed, placed],
        ),
        out_shape=[out, out],
        compiler_params=pltpu.CompilerParams(dimension_semantics=("arbitrary",)),
    )(order, own_hidden, other_hidden, own, other)


def sum_over_head(away, keep):
    bit = 1
    total, other = keep, away
    while bit < lax.axis_size("head"):
        came = exchange(other, "head", bit)
        total = total.astype(jnp.float32) + came.astype(jnp.float32)
        other = total.astype(jnp.bfloat16)
        bit *= 2
        if bit < lax.axis_size("head"):
            total = other
    return total


def slab_routes(bands, mesh_rows):
    reach = (WINDOW + mesh_rows - 2) // mesh_rows
    if bands <= 2 * reach + 1:
        offsets = list(range(1, bands))
        return True, offsets, [[(i, (i - o) % bands) for i in range(bands)] for o in offsets]
    offsets = [sign * step for step in range(1, reach + 1) for sign in (1, -1)]
    routes = [[(i, i - o) for i in range(bands) if 0 <= i - o < bands] for o in offsets]
    return False, offsets, routes


def slab_ids(window_ids, mesh_rows, offsets, around):
    bands = lax.axis_size("band")
    key_ids = []
    for offset in [0] + offsets:
        source = lax.axis_index("band") + offset
        if around:
            source = source % bands
        inside = (source >= 0) & (source < bands)
        safe = jnp.clip(source, 0, bands - 1)
        ids = lax.dynamic_slice_in_dim(window_ids, safe * mesh_rows, mesh_rows, 0)
        key_ids.append(jnp.where(inside, ids, -1).reshape(1, mesh_rows))
    query_ids = lax.dynamic_slice_in_dim(
        window_ids, lax.axis_index("band") * mesh_rows, mesh_rows, 0
    ).reshape(mesh_rows, 1)
    return query_ids, jnp.stack(key_ids)


def paired_device(
    grid_feats,
    mesh_feats,
    enc_in,
    enc_out,
    proc_in,
    proc_out,
    ff_up,
    ff_down,
    dec_in,
    dec_out,
    enc_list,
    enc_count,
    dec_list,
    dec_count,
    window_ids,
):
    bands = lax.axis_size("band")
    heads = lax.axis_size("head")
    band_index = lax.axis_index("band")
    head_index = lax.axis_index("head")
    side = head_index % 2
    grid_rows = grid_feats.shape[0]
    mesh_rows = mesh_feats.shape[0]
    grid_blocks = grid_rows // BLOCK
    mesh_blocks = mesh_rows // BLOCK
    half_blocks = mesh_blocks // 2
    turns = jnp.arange(mesh_blocks, dtype=jnp.int32)
    order = (turns + (1 - side) * half_blocks) % mesh_blocks
    barrier = lax.optimization_barrier
    kv_cols, q_cols = (0, 2 * LANES), (2 * LANES, LANES)
    o_start = 3 * LANES

    enc_kv_pieces = from_bands(
        jnp.concatenate([whole_pack(enc_in, enc_out, "kv", o) for o in (False, True)], axis=1),
    )
    enc_qo_own = from_bands(whole_pack(enc_in, enc_out, "qo", False))
    enc_qo_other = [whole_pack(enc_in, enc_out, "qo", True)]
    for piece in enc_qo_own[1:]:
        enc_qo_other.append(swap(piece))
    enc_bias = list_bias(enc_list, enc_count, band_index, mesh_blocks, grid_blocks)
    dec_bias = list_bias(dec_list, dec_count, band_index, grid_blocks, mesh_blocks)
    around, offsets, routes = slab_routes(bands, mesh_rows)
    query_ids, key_ids = slab_ids(window_ids, mesh_rows, offsets, around)

    grid_norm = normed(grid_feats)
    mesh_norm = normed(mesh_feats)

    (enc_kv,) = project_placed(grid_norm, [enc_kv_pieces], 4 * LANES, False)
    early = barrier(
        (
            pack(proc_in, proc_out, "kvqo"),
            own_half(ff_up, 1),
            own_half(ff_down, 0),
            pack(dec_in, dec_out, "kvqo"),
            enc_kv,
        )
    )
    proc_own, up_own, down_own = [band_gather(value) for value in early[:3]]
    dec_half = early[3]
    proc_other = swap(proc_own)
    up_other = swap(up_own)
    down_other = swap(down_own)
    low, high = neighbours(enc_kv)
    enc_q, qo_own, qo_other = project_placed(
        mesh_norm, [enc_qo_own, enc_qo_other], LANES, True
    )
    away, keep = attend_pair(
        enc_q, [low, enc_kv, high], [enc_bias], False, [qo_own, qo_other], LANES, order
    )
    state = half_of(mesh_feats, side).astype(jnp.float32) + sum_over_head(away, keep)

    mine = normed(state)
    theirs = exchange(mine, "head", 1)
    proc_kv, proc_q = project_pair(
        mine, theirs, side, proc_own, proc_other, [kv_cols, q_cols]
    )
    slab = [proc_kv] + [lax.ppermute(proc_kv, "band", route) for route in routes]
    dec_own = band_gather(barrier((dec_half, *slab[1:]))[0])
    dec_other = swap(dec_own)
    away, keep = attend_pair(
        proc_q, slab, [query_ids, key_ids], True, [proc_own, proc_other], o_start, order
    )
    state = state + sum_over_head(away, keep)

    mine = normed(state)
    ff_norm = jnp.concatenate([exchange(mine, "head", 1), mine], axis=0)
    hidden = [gelu(dot(ff_norm, up)).astype(jnp.bfloat16) for up in (up_own, up_other)]
    away, keep = down_pair(*hidden, down_own, down_other, jnp.arange(2, dtype=jnp.int32))
    state = state + sum_over_head(away, keep)

    mine = normed(state)
    theirs = exchange(mine, "head", 1)
    (dec_kv,) = project_pair(mine, theirs, side, dec_own, dec_other, [kv_cols])
    grid_half = grid_rows // 2
    (dec_q,) = project_pair(
        grid_norm[:grid_half],
        grid_norm[grid_half:],
        jnp.zeros((), jnp.int32),
        dec_own,
        dec_other,
        [q_cols],
    )
    low, high = neighbours(dec_kv)
    share = grid_rows // heads
    by_core = turns.reshape(-1, 2, share // BLOCK).transpose(1, 0, 2).reshape(2, -1)
    dec_order = jnp.where(side == 0, by_core[::-1].reshape(-1), by_core.reshape(-1))
    away, keep = attend_pair(
        dec_q, [low, dec_kv, high], [dec_bias], False, [dec_own, dec_other], o_start, dec_order
    )
    total = keep.astype(jnp.float32) + exchange(away, "head", 1).astype(jnp.float32)
    bit = 2
    position = head_index // 2
    while bit < heads:
        parts = total.reshape(-1, 2, share, total.shape[1])
        mine = position % 2
        send = lax.dynamic_index_in_dim(parts, 1 - mine, 1, keepdims=False)
        kept = lax.dynamic_index_in_dim(parts, mine, 1, keepdims=False)
        got = exchange(send.astype(jnp.bfloat16), "head", bit)
        total = (
            kept.astype(jnp.bfloat16).astype(jnp.float32) + got.astype(jnp.float32)
        ).reshape(-1, total.shape[1])
        position = position // 2
        bit *= 2
    residual = lax.dynamic_slice_in_dim(grid_feats, head_index * share, share, 0)
    return (residual.astype(jnp.float32) + total).astype(jnp.bfloat16)


def body(*args):
    w_in, w_out = args[2], args[3]
    paired = (
        lax.axis_size("members") == 2
        and w_in.shape[2] == 4 * HD
        and 2 * HD == LANES
        and w_in.shape[1] == w_out.shape[1]
        and w_in.shape[1] % LANES == 0
        and args[0].shape[0] % (lax.axis_size("head") * BLOCK) == 0
        and args[0].shape[0] == args[1].shape[0]
    )
    if not paired:
        return per_device(*args)
    return paired_device(*args)


def solution(mesh):
    return jax.shard_map(
        body,
        mesh=mesh,
        in_specs=(
            P(("members", "band"), None),
            P(("members", "band"), None),
            P(None, "band", "head"),
            P("head", "band"),
            P(None, "band", "head"),
            P("head", "band"),
            P("band", "head"),
            P("head", "band"),
            P(None, "band", "head"),
            P("head", "band"),
            P(),
            P(),
            P(),
            P(),
            P(),
        ),
        out_specs=P(("members", "band", "head"), None),
        check_vma=False,
    )
```
